32 devices in a mesh: row: 8 (over y, x, core), col: 4 (over z).
Axes of the slice: x: 2, y: 2, z: 4, core: 2. Of those that a mesh axis runs over, the one named last changes fastest.
Arguments:
- entities: bfloat16 [2, 32768, 200], P(None, ('row', 'col')), may hold values from -2.390625 to 2.390625
- relations: bfloat16 [2, 1024, 200], replicated, may hold values from -6 to 6
- src_index: int32 [131072], P(('row', 'col')), may hold values from 0 to 4095
- dst_index: int32 [131072], P(('row', 'col')), may hold values from 0 to 8191
- rel_index: int32 [131072], P(('row', 'col')), may hold values from 0 to 1023
- neg_block: int32 [256], P(('row', 'col')), may hold values from 0 to 15
Outputs:
- edge_loss: float32 [131072], P(('row', 'col'))
- relation_grad: float32 [2, 1024, 200], P(None, ('row', 'col'))
The draws below stay inside these ranges and needn't reach their ends.
All inputs are finite; a program needn't handle non-finite values.
Results may differ from the reference program's by a relative error of at most 0.0018.
Values may be sent and summed in bfloat16 or wider, within the bound.
A program may use at most 128 MiB of HBM per device.

```python
import jax
import jax.numpy as jnp
from jax import lax

DIM = 200
NREL = 1024
ENT_DEV = 1024
EDGE_DEV = 4096
GROUP = 512
NEGB = 512
NENT = 32768
EDGES = 131072
N_ROW = 8
N_COL = 4


def place_ends(entries, rng, least, largest):
    longest = entries.shape.index(max(entries.shape))
    spots = []
    for shift in (0, 1):
        where = [jax.random.randint(jax.random.fold_in(rng, axis), (), 0, length) for axis, length in enumerate(entries.shape)]
        where[longest] = (where[longest] + shift) % entries.shape[longest]
        spots.append(tuple(where))
    return entries.at[spots[0]].set(least).at[spots[1]].set(largest)


def block_levels(rng, shape, cuts, low, high):
    loudness, own = 1.0, jax.random.fold_in(rng, 6)
    for dim, parts in cuts:
        steps = jnp.exp(jax.random.uniform(jax.random.fold_in(own, dim), (parts,), jnp.float32, low / len(cuts), high / len(cuts)))
        loudness = loudness * jnp.repeat(steps, shape[dim] // parts).reshape([-1 if axis == dim else 1 for axis in range(len(shape))])
    return loudness


def centred(stream_key, extent, width, bound, pieces=(), kind=jnp.bfloat16):
    level = block_levels(stream_key, extent, pieces, -0.22, 0.18) if pieces else 1.0
    array = jax.random.normal(stream_key, extent, jnp.float32) * width * level
    return jnp.minimum(jnp.maximum(array, -bound), bound).astype(kind)


def setup_inputs(seed: int = 0) -> dict:
    key_of = jax.random.split(jax.random.key(seed), 7)
    return {
        "entities": centred(key_of[0], (2, NENT, DIM), 0.4, 2.390625, ((1, 32),)),
        "relations": centred(key_of[1], (2, NREL, DIM), 1.0, 6.0),
        "src_index": place_ends(jax.random.randint(key_of[2], (EDGES,), 0, N_COL * ENT_DEV), jax.random.fold_in(key_of[2], 1), 0, (N_COL * ENT_DEV) - 1).astype(jnp.int32),
        "dst_index": place_ends(jax.random.randint(key_of[3], (EDGES,), 0, N_ROW * ENT_DEV), jax.random.fold_in(key_of[3], 1), 0, (N_ROW * ENT_DEV) - 1).astype(jnp.int32),
        "rel_index": place_ends(jax.random.randint(key_of[4], (EDGES,), 0, NREL), jax.random.fold_in(key_of[4], 1), 0, NREL - 1).astype(jnp.int32),
        "neg_block": place_ends(jax.random.randint(key_of[5], (EDGES // GROUP,), 0, N_ROW * ENT_DEV // NEGB), jax.random.fold_in(key_of[5], 1), 0, (N_ROW * ENT_DEV // NEGB) - 1).astype(jnp.int32),
    }


def bucket_terms(picked_src, picked_dst, negatives, relations, rel_ids):
    onehot = (rel_ids[:, None] == jnp.arange(relations.shape[1], dtype=jnp.int32)[None, :]).astype(jnp.bfloat16)
    rel_re = jnp.dot(onehot, relations[0], preferred_element_type=jnp.float32)
    rel_im = jnp.dot(onehot, relations[1], preferred_element_type=jnp.float32)
    src_re = picked_src[0].astype(jnp.float32)
    src_im = picked_src[1].astype(jnp.float32)
    dst_re = picked_dst[0].astype(jnp.float32)
    dst_im = picked_dst[1].astype(jnp.float32)
    query_re = src_re * rel_re - src_im * rel_im
    query_im = src_re * rel_im + src_im * rel_re
    pos_score = jnp.sum(query_re * dst_re, 1) + jnp.sum(query_im * dst_im, 1)
    groups = negatives.shape[1]
    dim = query_re.shape[1]
    qre_f = query_re.astype(jnp.bfloat16).astype(jnp.float32).reshape(groups, -1, dim)
    qim_f = query_im.astype(jnp.bfloat16).astype(jnp.float32).reshape(groups, -1, dim)
    neg_re = negatives[0].astype(jnp.float32)
    neg_im = negatives[1].astype(jnp.float32)
    neg_score = jnp.einsum("kcd,knd->kcn", qre_f, neg_re, precision=lax.Precision.HIGHEST) + jnp.einsum("kcd,knd->kcn", qim_f, neg_im, precision=lax.Precision.HIGHEST)
    edge_loss = jax.nn.softplus(-pos_score) + jnp.mean(jax.nn.softplus(neg_score), -1).reshape(-1)
    weights = (jax.nn.sigmoid(neg_score) / NEGB).astype(jnp.bfloat16).astype(jnp.float32)
    gneg_re = jnp.einsum("kcn,knd->kcd", weights, neg_re, precision=lax.Precision.HIGHEST).reshape(-1, dim)
    gneg_im = jnp.einsum("kcn,knd->kcd", weights, neg_im, precision=lax.Precision.HIGHEST).reshape(-1, dim)
    pull = jax.nn.sigmoid(-pos_score)[:, None]
    grad_re = gneg_re - pull * dst_re
    grad_im = gneg_im - pull * dst_im
    term_re = (grad_re * src_re + grad_im * src_im).astype(jnp.bfloat16)
    term_im = (grad_im * src_re - grad_re * src_im).astype(jnp.bfloat16)
    dims = (((0,), (0,)), ((), ()))
    rel_grad = jnp.stack([lax.dot_general(onehot, term_re, dims, preferred_element_type=jnp.float32), lax.dot_general(onehot, term_im, dims, preferred_element_type=jnp.float32)], 0)
    return edge_loss, rel_grad


def reference(entities, relations, src_index, dst_index, rel_index, neg_block):
    dim = entities.shape[2]
    grid_rows = entities.reshape(2, N_ROW, N_COL, ENT_DEV, dim)
    groups = EDGE_DEV // GROUP

    def visit(accum, device):
        row_pos = device // N_COL
        col_pos = device % N_COL
        source_rows = lax.dynamic_index_in_dim(grid_rows, row_pos, 1, keepdims=False).reshape(2, N_COL * ENT_DEV, dim)
        target_rows = lax.dynamic_index_in_dim(grid_rows, col_pos, 2, keepdims=False).reshape(2, N_ROW * ENT_DEV, dim)
        sources = lax.dynamic_slice_in_dim(src_index, (device * EDGE_DEV).astype(jnp.int32), EDGE_DEV)
        targets = lax.dynamic_slice_in_dim(dst_index, (device * EDGE_DEV).astype(jnp.int32), EDGE_DEV)
        rel_ids = lax.dynamic_slice_in_dim(rel_index, (device * EDGE_DEV).astype(jnp.int32), EDGE_DEV)
        block_ids = lax.dynamic_slice_in_dim(neg_block, (device * groups).astype(jnp.int32), groups)
        picked_src = jnp.take(source_rows, sources, axis=1)
        picked_dst = jnp.take(target_rows, targets, axis=1)
        negatives = jnp.take(target_rows.reshape(2, -1, NEGB, dim), block_ids, axis=1)
        edge_loss, rel_grad = bucket_terms(picked_src, picked_dst, negatives, relations, rel_ids)
        return accum + rel_grad, edge_loss

    rel_total, losses = lax.scan(visit, jnp.zeros((2, NREL, dim), jnp.float32), jnp.arange(N_ROW * N_COL, dtype=jnp.int32))
    return losses.reshape(-1), rel_total
```

```python
import functools

import jax
import jax.numpy as jnp
from jax import lax
from jax.experimental import pallas as pl
from jax.experimental.pallas import tpu as pltpu
from jax.sharding import PartitionSpec as P

NEGB = 512
LANE = 128
WIDE = 256
MESH = pl.DeviceIdType.MESH
F32 = jnp.float32
BF16 = jnp.bfloat16
PICKS = 32
QROWS = 32


def log1p_small(u):
    return jnp.where(u < 2.0**-9, u - 0.5 * u * u, jnp.log(1.0 + u))


def step_kernel(
    n_col, group, src_i, dst_i, rel_i, neg_i, rel_row, ent, rel, loss, grad,
    srcb, dstb, relb, s_tab, o_tab, w_tab, gs, go, gw, qb, pos, key, acc, pairb, tot, inb, zs, zin,
    loc_sem, send_sem, recv_sem,
):
    r, c = lax.axis_index("row"), lax.axis_index("col")
    chip, core = r // 2, r % 2
    y, x = chip // 2, chip % 2
    row_of = lambda yy, xx, k: (yy * 2 + xx) * 2 + k
    xr, yr, dr = row_of(y, 1 - x, core), row_of(1 - y, x, core), row_of(1 - y, 1 - x, core)
    mr, mx, my, md = (row_of(yy, xx, 1 - core) for yy, xx in ((y, x), (y, 1 - x), (1 - y, x), (1 - y, 1 - x)))
    mate, xp, yp, dp = (mr, c), (xr, c), (yr, c), (dr, c)
    dim, count = ent.shape[1], ent.shape[2]
    n_rel = rel.shape[2]
    groups = neg_i.shape[0]
    per = count // NEGB
    rest = dim - LANE

    barrier = pltpu.get_barrier_semaphore()
    peers = [mate, xp, yp, dp] + [(r, (c + b) % n_col) for b in range(1, n_col)]
    for peer in peers:
        pl.semaphore_signal(barrier, inc=1, device_id=peer, device_id_type=MESH)
    pl.semaphore_wait(barrier, len(peers))

    started = []

    def copy(k, src, dst, peer):
        return pltpu.make_async_remote_copy(
            src_ref=src, dst_ref=dst, send_sem=send_sem.at[k], recv_sem=recv_sem.at[k],
            device_id=peer, device_id_type=MESH,
        )

    def start(k, src, dst, peer):
        move = copy(k, src, dst, peer)
        move.start()
        started.append((None, move))

    def arrive(k, dst):
        copy(k, dst, dst, mate).wait_recv()

    own = lambda p: ent.at[:, :, p * NEGB : (p + 1) * NEGB]
    inside = lambda v: jnp.logical_and(v >= 0, v < n_col)

    def line_id(way, age, part):
        return ((0 if way > 0 else n_col - 1) + age) * 2 + part

    def line_send(way, age, part):
        shard = c - way * age
        cond = jnp.logical_and(inside(c + way), inside(shard))
        src = own(part) if age == 0 else srcb.at[shard * per + part]
        move = copy(line_id(way, age, part), src, srcb.at[shard * per + part], (r, c + way))

        @pl.when(cond)
        def _():
            move.start()

        started.append((cond, move))

    def line_wait(way, age, part):
        shard = c - way * (age + 1)

        @pl.when(inside(shard))
        def _():
            arrive(line_id(way, age, part), srcb.at[shard * per + part])

    base = 4 * (n_col - 1)
    X0, X1, Y0, Y1, XD, YD, M0 = (base + k for k in range(7))
    at_dst = lambda i, p: dstb.at[i * per + p]

    line_send(1, 0, 0)
    line_send(-1, 0, 0)
    start(X0, own(0), at_dst(r, 0), xp)
    start(Y1, own(1), at_dst(r, 1), yp)
    local_rel = pltpu.make_async_copy(rel, relb, loc_sem.at[0])
    local_ent = [pltpu.make_async_copy(own(p), at_dst(r, p), loc_sem.at[1 + p]) for p in range(per)]
    local_rel.start()
    for move in local_ent:
        move.start()
    line_send(1, 0, 1)
    line_send(-1, 0, 1)
    start(X1, own(1), at_dst(r, 1), xp)
    start(Y0, own(0), at_dst(r, 0), yp)
    start(M0, own(0), at_dst(r, 0), mate)
    start(M0 + 1, own(1), at_dst(r, 1), mate)

    def fill(read, targets):
        def step(j, carry):
            col = pl.multiple_of(j * LANE, LANE)
            for part in range(2):
                low = read(part, slice(0, LANE), col).astype(F32).T
                high = read(part, slice(LANE, dim), col).astype(F32)
                high = jnp.concatenate([high, jnp.zeros((LANE - rest, LANE), F32)], 0).T
                for table, first, _ in targets:
                    flat = table.reshape(table.shape[0] * 4, LANE)
                    at = first + col * 4 + part * 2
                    flat[pl.ds(at, LANE, stride=4), :] = low
                    flat[pl.ds(at + 1, LANE, stride=4), :] = high
            return carry

        lax.fori_loop(0, targets[0][2] // LANE, step, 0)

    def fill_half(buf, half, *tables):
        fill(
            lambda p, rows, col: buf[half, p, rows, pl.ds(col, LANE)],
            [(table, shard * (NEGB * 4), NEGB) for table, shard in tables],
        )

    def fill_dst(shard):
        for p in range(per):
            half = shard * per + p
            fill_half(dstb, half, (o_tab, half))

    def fill_src(shard):
        @pl.when(inside(shard))
        def _():
            for p in range(per):
                half = shard * per + p
                fill_half(srcb, half, (s_tab, half))

    def pick(table, index, g):
        def step(i, carry):
            got = []
            for u in range(PICKS):
                got.append(table[index[g * group + i * PICKS + u]])
            for u in range(PICKS):
                gs[pl.ds(pl.multiple_of((i * PICKS + u) * 4, 4), 4), :] = got[u]
            return carry

        lax.fori_loop(0, group // PICKS, step, 0)

    def pick_all(table, index, out):
        def one(g, carry):
            pick(table, index, g)

            def pack(i, inner):
                row = pl.multiple_of(i * QROWS, QROWS)
                at = pl.ds(pl.multiple_of(g * group + row, QROWS), QROWS)
                for k in range(4):
                    out[at, k * LANE : (k + 1) * LANE] = gs[pl.ds(row * 4 + k, QROWS, stride=4), :].astype(BF16)
                return inner

            lax.fori_loop(0, group // QROWS, pack, 0)
            return carry

        lax.fori_loop(0, groups, one, 0)

    rel_ids = rel_row[...]
    span = n_rel // (8 * n_col)
    row_part = lax.div(rel_ids, n_col * span)
    key[...] = (
        lax.rem(lax.div(rel_ids, span), n_col) * (8 * span)
        + lax.rem(row_part, 2) * (4 * span) + lax.div(row_part, 2) * span + lax.rem(rel_ids, span)
    )

    local_rel.wait()
    fill(lambda p, rows, col: relb[p, rows, pl.ds(col, LANE)], [(w_tab, 0, n_rel)])
    pick_all(w_tab, rel_i, gw)
    for move in local_ent:
        move.wait()
    for p in range(per):
        fill_half(dstb, r * per + p, (o_tab, r * per + p), (s_tab, c * per + p))

    arrive(X0, at_dst(xr, 0))
    start(YD, at_dst(xr, 0), at_dst(xr, 0), yp)
    arrive(Y1, at_dst(yr, 1))
    start(XD, at_dst(yr, 1), at_dst(yr, 1), xp)
    for way in (1, -1):
        line_wait(way, 0, 0)
        line_send(way, 1, 0)
    start(M0 + 2, at_dst(xr, 0), at_dst(xr, 0), mate)
    start(M0 + 3, at_dst(yr, 1), at_dst(yr, 1), mate)
    arrive(M0, at_dst(mr, 0))
    arrive(M0 + 1, at_dst(mr, 1))
    fill_dst(mr)

    arrive(X1, at_dst(xr, 1))
    start(M0 + 4, at_dst(xr, 1), at_dst(xr, 1), mate)
    arrive(Y0, at_dst(yr, 0))
    start(M0 + 5, at_dst(yr, 0), at_dst(yr, 0), mate)
    for way in (1, -1):
        line_wait(way, 0, 1)
        line_send(way, 1, 1)
    fill_dst(xr)
    fill_dst(yr)
    fill_src(c - 1)
    fill_src(c + 1)
    arrive(M0 + 2, at_dst(mx, 0))
    arrive(M0 + 4, at_dst(mx, 1))
    fill_dst(mx)
    arrive(M0 + 3, at_dst(my, 1))
    arrive(M0 + 5, at_dst(my, 0))
    fill_dst(my)

    arrive(YD, at_dst(dr, 0))
    start(M0 + 6, at_dst(dr, 0), at_dst(dr, 0), mate)
    arrive(XD, at_dst(dr, 1))
    start(M0 + 7, at_dst(dr, 1), at_dst(dr, 1), mate)
    for way in (1, -1):
        line_wait(way, 1, 0)
        line_send(way, 2, 0)
    fill_dst(dr)
    arrive(M0 + 6, at_dst(md, 0))
    arrive(M0 + 7, at_dst(md, 1))
    fill_dst(md)
    pick_all(o_tab, dst_i, go)

    for way in (1, -1):
        line_wait(way, 1, 1)
        line_send(way, 2, 1)
    fill_src(c - 2)
    fill_src(c + 2)
    for way in (1, -1):
        line_wait(way, 2, 0)
        line_wait(way, 2, 1)
    fill_src(c - 3)
    fill_src(c + 3)

    eye = lax.broadcasted_iota(jnp.int32, (LANE, LANE), 0) == lax.broadcasted_iota(jnp.int32, (LANE, LANE), 1)
    nt = (((1,), (1,)), ((), ()))
    cuts = ((0, LANE), (LANE, dim))

    def one_group(g, carry):
        pick(s_tab, src_i, g)

        def query(i, inner):
            row = pl.multiple_of(i * QROWS, QROWS)
            rows = pl.ds(pl.multiple_of(g * group + row, QROWS), QROWS)
            score = None
            for half, (low, high) in enumerate(cuts):
                near = lambda p: gs[pl.ds(row * 4 + p * 2 + half, QROWS, stride=4), :]
                dense = lambda ref, p: ref[rows, p * WIDE + half * LANE : p * WIDE + (half + 1) * LANE].astype(F32)
                sr, si, wr, wi = near(0), near(1), dense(gw, 0), dense(gw, 1)
                qr = sr * wr - si * wi
                qi = sr * wi + si * wr
                add = qr * dense(go, 0) + qi * dense(go, 1)
                score = add if score is None else score + add
                qb[0, pl.ds(row, QROWS), low:high] = qr[:, : high - low].astype(BF16)
                qb[1, pl.ds(row, QROWS), low:high] = qi[:, : high - low].astype(BF16)
            pos[pl.ds(row, QROWS), :] = jnp.sum(score, 1, keepdims=True)
            return inner

        lax.fori_loop(0, group // QROWS, query, 0)

        b = neg_i[g]
        near = lambda p: dstb[b, p]
        score = jnp.dot(qb[0], near(0), preferred_element_type=F32)
        score = score + jnp.dot(qb[1], near(1), preferred_element_type=F32)
        small = jnp.exp(-jnp.abs(score))
        soft = jnp.maximum(score, 0.0) + log1p_small(small)
        turn = 1.0 / (1.0 + small)
        weight = jnp.where(score >= 0.0, turn, small * turn).astype(BF16)
        p = pos[...]
        p_small = jnp.exp(-jnp.abs(p))
        value = jnp.maximum(-p, 0.0) + log1p_small(p_small) + jnp.sum(soft, 1, keepdims=True) * (1.0 / NEGB)
        pull = jnp.where(p >= 0.0, p_small, 1.0) / (1.0 + p_small)
        for i in range(group // LANE):
            piece = value[i * LANE : (i + 1) * LANE]
            loss[pl.ds(g * (group // LANE) + i, 1), :] = jnp.sum(jnp.where(eye, piece, 0.0), 0, keepdims=True)
        g_re = lax.dot_general(weight, near(0), nt, preferred_element_type=F32) * (1.0 / NEGB)
        g_im = lax.dot_general(weight, near(1), nt, preferred_element_type=F32) * (1.0 / NEGB)
        rows = pl.ds(pl.multiple_of(g * group, group), group)
        for half, (low, high) in enumerate(cuts):
            wide = high - low
            part = lambda q: gs[pl.ds(q * 2 + half, group, stride=4), :][:, :wide]
            lanes = lambda q: slice(q * WIDE + low, q * WIDE + high)
            d_re = g_re[:, low:high] - pull * go[rows, lanes(0)].astype(F32)
            d_im = g_im[:, low:high] - pull * go[rows, lanes(1)].astype(F32)
            s_re, s_im = part(0), part(1)
            gw[rows, lanes(0)] = (d_re * s_re + d_im * s_im).astype(BF16)
            gw[rows, lanes(1)] = (d_im * s_re - d_re * s_im).astype(BF16)
        return carry

    lax.fori_loop(0, groups, one_group, 0)

    tile = 8 * span
    edges = gw.shape[0]
    home = [2, 1, 3, 0]
    S0 = M0 + 8
    spots = [(xp, (y * 2 + 1 - x)), (yp, ((1 - y) * 2 + x)), (dp, ((1 - y) * 2 + 1 - x))]
    order = [2, 0, 1]

    def pair_up(t):
        arrive(S0 + t, pairb.at[t])
        tot[t] = acc[t, core] + pairb[t]
        for k in order:
            peer, there = spots[k]
            start(S0 + 4 + t * 3 + k, tot.at[t, there], inb.at[t, k], peer)

    def plane_sum(t):
        total = tot[t, chip]
        for k in range(3):
            arrive(S0 + 4 + t * 3 + k, inb.at[t, k])
            total = total + inb[t, k]
        return total

    for t in range(n_col):
        plane = (c + home[t]) % n_col
        ids = lax.broadcasted_iota(jnp.int32, (tile, edges), 0) + plane * tile
        hot = jnp.where(ids == key[...], 1.0, 0.0).astype(BF16)
        acc[t] = jnp.dot(hot, gw[...], preferred_element_type=F32).reshape(2, 4, span, 2 * WIDE)
        start(S0 + t, acc.at[t, 1 - core], pairb.at[t], mate)
        if t:
            pair_up(t - 1)
    pair_up(n_col - 1)
    Z0 = S0 + 4 + n_col * 3
    for t in range(n_col - 1):
        zs[t] = plane_sum(t)
        start(Z0 + t, zs.at[t], zin.at[t], (r, (c + home[t]) % n_col))
    total = plane_sum(n_col - 1)
    for t in range(n_col - 1):
        arrive(Z0 + t, zin.at[t])
        total = total + zin[t]
    grad[0] = total[:, :dim]
    grad[1] = total[:, WIDE : WIDE + dim]

    for cond, move in started:
        if cond is None:
            move.wait_send()
        else:
            pl.when(cond)(move.wait_send)


def step_call(n_row, n_col, ent, rel, src_index, dst_index, rel_index, neg_block):
    edges, groups = src_index.shape[0], neg_block.shape[0]
    group = edges // groups
    parts, dim, count = ent.shape
    n_rel = rel.shape[2]
    span = n_rel // (n_row * n_col)
    chips = n_row // 2
    smem = pl.BlockSpec(memory_space=pltpu.SMEM)
    vmem = pl.BlockSpec(memory_space=pltpu.VMEM)
    hbm = pl.BlockSpec(memory_space=pltpu.HBM)
    dma = pltpu.SemaphoreType.DMA
    copies = 4 * (n_col - 1) + 14 + 4 + n_col * 3 + n_col - 1
    return pl.pallas_call(
        functools.partial(step_kernel, n_col, group),
        name="step",
        out_shape=(
            jax.ShapeDtypeStruct((edges // LANE, LANE), F32),
            jax.ShapeDtypeStruct((parts, span, dim), F32),
        ),
        in_specs=[smem, smem, smem, smem, vmem, hbm, hbm],
        out_specs=(vmem, vmem),
        scratch_shapes=[
            pltpu.VMEM((n_col * count // NEGB, parts, dim, NEGB), BF16),
            pltpu.VMEM((n_row * count // NEGB, parts, dim, NEGB), BF16),
            pltpu.VMEM(rel.shape, BF16),
            pltpu.VMEM((n_col * count, 4, LANE), F32),
            pltpu.VMEM((n_row * count, 4, LANE), F32),
            pltpu.VMEM((n_rel, 4, LANE), F32),
            pltpu.VMEM((group * 4, LANE), F32),
            pltpu.VMEM((edges, 2 * WIDE), BF16),
            pltpu.VMEM((edges, 2 * WIDE), BF16),
            pltpu.VMEM((parts, group, dim), BF16),
            pltpu.VMEM((group, 1), F32),
            pltpu.VMEM((1, edges), jnp.int32),
            pltpu.VMEM((n_col, 2, chips, span, 2 * WIDE), F32),
            pltpu.VMEM((n_col, chips, span, 2 * WIDE), F32),
            pltpu.VMEM((n_col, chips, span, 2 * WIDE), F32),
            pltpu.VMEM((n_col, 3, span, 2 * WIDE), F32),
            pltpu.VMEM((n_col - 1, span, 2 * WIDE), F32),
            pltpu.VMEM((n_col - 1, span, 2 * WIDE), F32),
            dma((3,)), dma((copies,)), dma((copies,)),
        ],
        compiler_params=pltpu.CompilerParams(
            collective_id=0, has_side_effects=True, vmem_limit_bytes=67043328
        ),
    )(src_index, dst_index, rel_index, neg_block, rel_index.reshape(1, edges), ent, rel)


def body(n_row, n_col, entities, relations, src_index, dst_index, rel_index, neg_block):
    dim = entities.shape[2]
    count = entities.shape[1]
    args = (entities, relations, src_index, dst_index, rel_index, neg_block)
    fits = LANE < dim < WIDE and (n_row + n_col) * count * 4 * LANE * 4 <= 26 * 2**20
    if n_row != 8 or n_col != 4 or count != 2 * NEGB or not fits:
        return wide_body(*args)
    flip = lambda a: jnp.transpose(a, (0, 2, 1))
    edge_loss, grad = step_call(
        n_row, n_col, flip(entities), flip(relations), src_index, dst_index, rel_index, neg_block
    )
    return edge_loss.reshape(-1), grad


def bucket_terms(picked_src, picked_dst, negatives, relations, rel_ids):
    onehot = (rel_ids[:, None] == jnp.arange(relations.shape[1], dtype=jnp.int32)[None, :]).astype(
        jnp.bfloat16
    )
    rel_re = jnp.dot(onehot, relations[0], preferred_element_type=jnp.float32)
    rel_im = jnp.dot(onehot, relations[1], preferred_element_type=jnp.float32)
    src_re = picked_src[0].astype(jnp.float32)
    src_im = picked_src[1].astype(jnp.float32)
    dst_re = picked_dst[0].astype(jnp.float32)
    dst_im = picked_dst[1].astype(jnp.float32)
    query_re = src_re * rel_re - src_im * rel_im
    query_im = src_re * rel_im + src_im * rel_re
    pos_score = jnp.sum(query_re * dst_re, 1) + jnp.sum(query_im * dst_im, 1)
    groups = negatives.shape[1]
    dim = query_re.shape[1]
    qre_b = query_re.astype(jnp.bfloat16).reshape(groups, -1, dim)
    qim_b = query_im.astype(jnp.bfloat16).reshape(groups, -1, dim)
    neg_score = jnp.einsum(
        "kcd,knd->kcn", qre_b, negatives[0], preferred_element_type=jnp.float32
    ) + jnp.einsum("kcd,knd->kcn", qim_b, negatives[1], preferred_element_type=jnp.float32)
    edge_loss = jax.nn.softplus(-pos_score) + jnp.mean(jax.nn.softplus(neg_score), -1).reshape(-1)
    weights = (jax.nn.sigmoid(neg_score) / NEGB).astype(jnp.bfloat16)
    gneg_re = jnp.einsum(
        "kcn,knd->kcd", weights, negatives[0], preferred_element_type=jnp.float32
    ).reshape(-1, dim)
    gneg_im = jnp.einsum(
        "kcn,knd->kcd", weights, negatives[1], preferred_element_type=jnp.float32
    ).reshape(-1, dim)
    pull = jax.nn.sigmoid(-pos_score)[:, None]
    grad_re = gneg_re - pull * dst_re
    grad_im = gneg_im - pull * dst_im
    term_re = (grad_re * src_re + grad_im * src_im).astype(jnp.bfloat16)
    term_im = (grad_im * src_re - grad_re * src_im).astype(jnp.bfloat16)
    dims = (((0,), (0,)), ((), ()))
    rel_grad = jnp.stack(
        [
            lax.dot_general(onehot, term_re, dims, preferred_element_type=jnp.float32),
            lax.dot_general(onehot, term_im, dims, preferred_element_type=jnp.float32),
        ],
        0,
    )
    return (edge_loss, rel_grad)


def wide_body(entities, relations, src_index, dst_index, rel_index, neg_block):
    dim = entities.shape[2]
    source_rows = lax.all_gather(entities, "col", axis=1, tiled=True)
    picked_src = jnp.take(source_rows, src_index, axis=1)
    target_rows = lax.all_gather(entities, "row", axis=1, tiled=True)
    picked_dst = jnp.take(target_rows, dst_index, axis=1)
    negatives = jnp.take(target_rows.reshape(2, -1, NEGB, dim), neg_block, axis=1)
    edge_loss, rel_grad = bucket_terms(picked_src, picked_dst, negatives, relations, rel_index)
    row_share = lax.psum_scatter(rel_grad, "row", scatter_dimension=1, tiled=True)
    grad_share = lax.psum_scatter(row_share, "col", scatter_dimension=1, tiled=True)
    return (edge_loss, grad_share)


def solution(mesh):
    placed = (
        P(None, ("row", "col"), None),
        P(),
        P(("row", "col")),
        P(("row", "col")),
        P(("row", "col")),
        P(("row", "col")),
    )
    return jax.shard_map(
        functools.partial(body, mesh.shape["row"], mesh.shape["col"]),
        mesh=mesh,
        in_specs=placed,
        out_specs=(P(("row", "col")), P(None, ("row", "col"), None)),
        check_vma=False,
    )
```

```python
import functools

import jax
import jax.numpy as jnp
from jax import lax
from jax.experimental import pallas as pl
from jax.experimental.pallas import tpu as pltpu
from jax.sharding import PartitionSpec as P

NEGB = 512
LANE = 128
WIDE = 256
MESH = pl.DeviceIdType.MESH
F32 = jnp.float32
BF16 = jnp.bfloat16
PICKS = 32
QROWS = 32


def log1p_small(u):
    return jnp.where(u < 2.0**-9, u - 0.5 * u * u, jnp.log(1.0 + u))


def step_kernel(
    n_col, group, stages, neg_i, src_row, dst_row, rel_row, ent, rel, loss, grad, late,
    srcb, dstb, relb, s_tab, o_tab, w_tab, gs, go, gw, qb, dots, key, spot, moved, order_v, order_s, lossp, flag,
    acc, pairb, tot, inb, zs, zin, loc_sem, send_sem, recv_sem,
):
    r, c = lax.axis_index("row"), lax.axis_index("col")
    chip, core = r // 2, r % 2
    y, x = chip // 2, chip % 2
    row_of = lambda yy, xx, k: (yy * 2 + xx) * 2 + k
    xr, yr, dr = row_of(y, 1 - x, core), row_of(1 - y, x, core), row_of(1 - y, 1 - x, core)
    mr, mx, my, md = (row_of(yy, xx, 1 - core) for yy, xx in ((y, x), (y, 1 - x), (1 - y, x), (1 - y, 1 - x)))
    mate, xp, yp, dp = (mr, c), (xr, c), (yr, c), (dr, c)
    dim, count = ent.shape[1], ent.shape[2]
    n_rel = rel.shape[2]
    groups = neg_i.shape[0]
    per = count // NEGB
    rest = dim - LANE

    barrier = pltpu.get_barrier_semaphore()
    peers = [mate, xp, yp, dp] + [(r, (c + b) % n_col) for b in range(1, n_col)]
    for peer in peers:
        pl.semaphore_signal(barrier, inc=1, device_id=peer, device_id_type=MESH)
    pl.semaphore_wait(barrier, len(peers))

    started = []

    def copy(k, src, dst, peer):
        return pltpu.make_async_remote_copy(
            src_ref=src, dst_ref=dst, send_sem=send_sem.at[k], recv_sem=recv_sem.at[k],
            device_id=peer, device_id_type=MESH,
        )

    def start(k, src, dst, peer):
        move = copy(k, src, dst, peer)
        move.start()
        started.append((None, move))

    def arrive(k, dst):
        copy(k, dst, dst, mate).wait_recv()

    own = lambda p: ent.at[:, :, p * NEGB : (p + 1) * NEGB]
    inside = lambda v: jnp.logical_and(v >= 0, v < n_col)

    def line_id(way, age, part):
        return ((0 if way > 0 else n_col - 1) + age) * 2 + part

    def line_send(way, age, part):
        shard = c - way * age
        cond = jnp.logical_and(inside(c + way), inside(shard))
        src = own(part) if age == 0 else srcb.at[shard * per + part]
        move = copy(line_id(way, age, part), src, srcb.at[shard * per + part], (r, c + way))

        @pl.when(cond)
        def _():
            move.start()

        started.append((cond, move))

    def line_wait(way, age, part):
        shard = c - way * (age + 1)

        @pl.when(inside(shard))
        def _():
            arrive(line_id(way, age, part), srcb.at[shard * per + part])

    base = 4 * (n_col - 1)
    X0, X1, Y0, Y1, XD, YD, M0 = (base + k for k in range(7))
    at_dst = lambda i, p: dstb.at[i * per + p]

    line_send(1, 0, 0)
    line_send(-1, 0, 0)
    start(X0, own(0), at_dst(r, 0), xp)
    start(Y1, own(1), at_dst(r, 1), yp)
    local_rel = pltpu.make_async_copy(rel, relb, loc_sem.at[0])
    local_ent = [pltpu.make_async_copy(own(p), at_dst(r, p), loc_sem.at[1 + p]) for p in range(per)]
    local_rel.start()
    for move in local_ent:
        move.start()
    line_send(1, 0, 1)
    line_send(-1, 0, 1)
    start(X1, own(1), at_dst(r, 1), xp)
    start(Y0, own(0), at_dst(r, 0), yp)
    start(M0, own(0), at_dst(r, 0), mate)
    start(M0 + 1, own(1), at_dst(r, 1), mate)

    def fill(read, targets):
        def step(j, carry):
            col = pl.multiple_of(j * LANE, LANE)
            for part in range(2):
                low = read(part, slice(0, LANE), col).astype(F32).T
                high = read(part, slice(LANE, dim), col).astype(F32)
                high = jnp.concatenate([high, jnp.zeros((LANE - rest, LANE), F32)], 0).T
                for table, first, _ in targets:
                    flat = table.reshape(table.shape[0] * 4, LANE)
                    at = first + col * 4 + part * 2
                    flat[pl.ds(at, LANE, stride=4), :] = low
                    flat[pl.ds(at + 1, LANE, stride=4), :] = high
            return carry

        lax.fori_loop(0, targets[0][2] // LANE, step, 0)

    def fill_half(buf, half, *tables):
        fill(
            lambda p, rows, col: buf[half, p, rows, pl.ds(col, LANE)],
            [(table, shard * (NEGB * 4), NEGB) for table, shard in tables],
        )

    def fill_dst(shard):
        for p in range(per):
            half = shard * per + p
            fill_half(dstb, half, (o_tab, half))

    def fill_src(shard):
        @pl.when(inside(shard))
        def _():
            for p in range(per):
                half = shard * per + p
                fill_half(srcb, half, (s_tab, half))

    def pick(table, kind, g, low, rows):
        top = table.shape[0] - 1
        keep = (lambda v: v & top) if top & (top + 1) == 0 else (lambda v: jnp.clip(v, 0, top))

        def step(i, carry):
            got = [table[keep(order_s[kind, g, low + i * PICKS + u])] for u in range(PICKS)]
            for u in range(PICKS):
                gs[pl.ds(pl.multiple_of((i * PICKS + u) * 4, 4), 4), :] = got[u]
            return carry

        lax.fori_loop(0, rows // PICKS, step, 0)

    def pick_all(table, kind, out):
        for low, rows in stages:
            def one(g, carry, low=low, rows=rows):
                pick(table, kind, g, low, rows)

                def pack(i, inner):
                    row = pl.multiple_of(i * QROWS, QROWS)
                    at = pl.ds(pl.multiple_of(groups * low + g * rows + row, QROWS), QROWS)
                    for k in range(4):
                        out[at, k * LANE : (k + 1) * LANE] = gs[pl.ds(row * 4 + k, QROWS, stride=4), :].astype(BF16)
                    return inner

                lax.fori_loop(0, rows // QROWS, pack, 0)
                return carry

            lax.fori_loop(0, groups, one, 0)

    span = n_rel // (8 * n_col)
    for g in range(groups):
        cut = slice(g * group, (g + 1) * group)
        for kind, ref in enumerate((src_row, dst_row, rel_row)):
            order_v[kind, g : g + 1, :] = ref[:, cut]
    halves = lax.div(order_v[0], NEGB)
    far = jnp.abs(lax.div(halves, per) - c) == n_col - 1
    last = jnp.logical_and(far, lax.rem(halves, per) == per - 1)
    early = jnp.where(far, 0.0, 1.0)
    middle = jnp.where(last, 0.0, 1.0) - early
    lane_id = lax.broadcasted_iota(jnp.int32, (groups, group), 1).astype(F32)
    before = lax.broadcasted_iota(jnp.int32, (group, group), 0) < lax.broadcasted_iota(jnp.int32, (group, group), 1)
    ahead = jnp.dot(
        jnp.concatenate([early, middle], 0).astype(BF16), jnp.where(before, 1.0, 0.0).astype(BF16),
        preferred_element_type=F32,
    )
    ahead0, ahead1 = ahead[:groups], ahead[groups:]
    n_early = jnp.sum(early, 1, keepdims=True)
    n_middle = jnp.sum(middle, 1, keepdims=True)
    place = jnp.where(
        far, jnp.where(last, n_early + n_middle + lane_id - ahead0 - ahead1, n_early + ahead1), ahead0
    )
    spot[...] = place.astype(jnp.int32)
    if len(stages) > 1:
        short = jnp.maximum(
            jnp.where(n_early < float(stages[1][0]), 1.0, 0.0),
            jnp.where(n_early + n_middle < float(stages[2][0]), 1.0, 0.0),
        )
        lanes = lax.broadcasted_iota(jnp.int32, (1, 2 * WIDE), 1)
        flag[...] = jnp.where(lanes == WIDE - 1, jnp.sum(short, 0, keepdims=True), 0.0)
    else:
        flag[...] = jnp.zeros_like(flag)

    def turn(g):
        ids = lax.broadcasted_iota(jnp.int32, (group, group), 0)
        return jnp.where(ids == spot[pl.ds(g, 1), :], 1.0, 0.0).astype(BF16)

    split = []
    for kind in range(3):
        split += [lax.div(order_v[kind], LANE), lax.rem(order_v[kind], LANE)]
    moved[...] = jnp.concatenate(split, 0).astype(F32)
    pieces = moved[...].astype(BF16)
    mine = lax.rem(lax.broadcasted_iota(jnp.int32, (6 * groups, group), 0), groups)
    nt = (((1,), (1,)), ((), ()))

    def reorder(g, carry):
        got = lax.dot_general(pieces, turn(g), nt, preferred_element_type=F32)
        moved[...] = jnp.where(mine == g, got, moved[...])
        return carry

    lax.fori_loop(0, groups, reorder, 0)
    for kind in range(3):
        at = kind * 2 * groups
        order_v[kind] = (moved[at : at + groups] * LANE + moved[at + groups : at + 2 * groups]).astype(jnp.int32)
    to_scalar = pltpu.make_async_copy(order_v, order_s, loc_sem.at[3])
    to_scalar.start()
    rel_ids = order_v[2]
    row_part = lax.div(rel_ids, n_col * span)
    keys = (
        lax.rem(lax.div(rel_ids, span), n_col) * (8 * span)
        + lax.rem(row_part, 2) * (4 * span) + lax.div(row_part, 2) * span + lax.rem(rel_ids, span)
    )
    for low, rows in stages:
        for g in range(groups):
            at = groups * low + g * rows
            key[:, at : at + rows] = keys[g : g + 1, low : low + rows]
    to_scalar.wait()

    local_rel.wait()
    fill(lambda p, rows, col: relb[p, rows, pl.ds(col, LANE)], [(w_tab, 0, n_rel)])
    pick_all(w_tab, 2, gw)
    for move in local_ent:
        move.wait()
    for p in range(per):
        fill_half(dstb, r * per + p, (o_tab, r * per + p), (s_tab, c * per + p))

    arrive(X0, at_dst(xr, 0))
    start(YD, at_dst(xr, 0), at_dst(xr, 0), yp)
    arrive(Y1, at_dst(yr, 1))
    start(XD, at_dst(yr, 1), at_dst(yr, 1), xp)
    for way in (1, -1):
        line_wait(way, 0, 0)
        line_send(way, 1, 0)
    start(M0 + 2, at_dst(xr, 0), at_dst(xr, 0), mate)
    start(M0 + 3, at_dst(yr, 1), at_dst(yr, 1), mate)
    arrive(M0, at_dst(mr, 0))
    arrive(M0 + 1, at_dst(mr, 1))
    fill_dst(mr)

    arrive(X1, at_dst(xr, 1))
    start(M0 + 4, at_dst(xr, 1), at_dst(xr, 1), mate)
    arrive(Y0, at_dst(yr, 0))
    start(M0 + 5, at_dst(yr, 0), at_dst(yr, 0), mate)
    for way in (1, -1):
        line_wait(way, 0, 1)
        line_send(way, 1, 1)
    fill_dst(xr)
    fill_dst(yr)
    fill_src(c - 1)
    fill_src(c + 1)
    arrive(M0 + 2, at_dst(mx, 0))
    arrive(M0 + 4, at_dst(mx, 1))
    fill_dst(mx)
    arrive(M0 + 3, at_dst(my, 1))
    arrive(M0 + 5, at_dst(my, 0))
    fill_dst(my)

    arrive(YD, at_dst(dr, 0))
    start(M0 + 6, at_dst(dr, 0), at_dst(dr, 0), mate)
    arrive(XD, at_dst(dr, 1))
    start(M0 + 7, at_dst(dr, 1), at_dst(dr, 1), mate)
    for way in (1, -1):
        line_wait(way, 1, 0)
        line_send(way, 2, 0)
    fill_dst(dr)
    arrive(M0 + 6, at_dst(md, 0))
    arrive(M0 + 7, at_dst(md, 1))
    fill_dst(md)
    pick_all(o_tab, 1, go)

    for way in (1, -1):
        line_wait(way, 1, 1)
        line_send(way, 2, 1)
    fill_src(c - 2)
    fill_src(c + 2)
    eye = lax.broadcasted_iota(jnp.int32, (LANE, LANE), 0) == lax.broadcasted_iota(jnp.int32, (LANE, LANE), 1)
    cuts = ((0, LANE), (LANE, dim))

    def main_stage(low_row, size):
        def one_group(g, carry):
            pick(s_tab, 0, g, low_row, size)
            first = groups * low_row + g * size

            def query(i, inner):
                row = pl.multiple_of(i * QROWS, QROWS)
                rows = pl.ds(pl.multiple_of(first + row, QROWS), QROWS)
                score = None
                for half, (low, high) in enumerate(cuts):
                    near = lambda p: gs[pl.ds(row * 4 + p * 2 + half, QROWS, stride=4), :]
                    dense = lambda ref, p: ref[rows, p * WIDE + half * LANE : p * WIDE + (half + 1) * LANE].astype(F32)
                    sr, si, wr, wi = near(0), near(1), dense(gw, 0), dense(gw, 1)
                    qr = sr * wr - si * wi
                    qi = sr * wi + si * wr
                    add = qr * dense(go, 0) + qi * dense(go, 1)
                    score = add if score is None else score + add
                    qb[0, pl.ds(row, QROWS), low:high] = qr[:, : high - low].astype(BF16)
                    qb[1, pl.ds(row, QROWS), low:high] = qi[:, : high - low].astype(BF16)
                dots[pl.ds(row, QROWS), :] = score
                return inner

            lax.fori_loop(0, size // QROWS, query, 0)
            b = neg_i[g]
            near = lambda p: dstb[b, p]
            score = jnp.dot(qb[0, :size], near(0), preferred_element_type=F32)
            score = score + jnp.dot(qb[1, :size], near(1), preferred_element_type=F32)
            small = jnp.exp(-jnp.abs(score))
            soft = jnp.maximum(score, 0.0) + log1p_small(small)
            ratio = 1.0 / (1.0 + small)
            weight = jnp.where(score >= 0.0, ratio, small * ratio).astype(BF16)
            p = jnp.sum(dots[:size], 1, keepdims=True)
            p_small = jnp.exp(-jnp.abs(p))
            value = jnp.maximum(-p, 0.0) + log1p_small(p_small) + jnp.sum(soft, 1, keepdims=True) * (1.0 / NEGB)
            pull = jnp.where(p >= 0.0, p_small, 1.0) / (1.0 + p_small)
            for i in range(size // LANE):
                piece = value[i * LANE : (i + 1) * LANE]
                lossp[pl.ds((low_row // LANE + i) * groups + g, 1), :] = jnp.sum(jnp.where(eye, piece, 0.0), 0, keepdims=True)
            g_re = lax.dot_general(weight, near(0), nt, preferred_element_type=F32) * (1.0 / NEGB)
            g_im = lax.dot_general(weight, near(1), nt, preferred_element_type=F32) * (1.0 / NEGB)
            rows = pl.ds(pl.multiple_of(first, size), size)
            for half, (low, high) in enumerate(cuts):
                wide = high - low
                part = lambda q: gs[pl.ds(q * 2 + half, size, stride=4), :][:, :wide]
                lanes = lambda q: slice(q * WIDE + low, q * WIDE + high)
                d_re = g_re[:, low:high] - pull * go[rows, lanes(0)].astype(F32)
                d_im = g_im[:, low:high] - pull * go[rows, lanes(1)].astype(F32)
                s_re, s_im = part(0), part(1)
                gw[rows, lanes(0)] = (d_re * s_re + d_im * s_im).astype(BF16)
                gw[rows, lanes(1)] = (d_im * s_re - d_re * s_im).astype(BF16)
            return carry

        lax.fori_loop(0, groups, one_group, 0)

    tile = 8 * span
    edges = gw.shape[0]

    def far_half(p):
        for way in (1, -1):
            line_wait(way, n_col - 2, p)
            shard = c - way * (n_col - 1)

            @pl.when(inside(shard))
            def _():
                fill_half(srcb, shard * per + p, (s_tab, shard * per + p))

    def terms(plane, low, high):
        ids = lax.broadcasted_iota(jnp.int32, (tile, high - low), 0) + plane * tile
        hot = jnp.where(ids == key[:, low:high], 1.0, 0.0).astype(BF16)
        return jnp.dot(hot, gw[low:high], preferred_element_type=F32)

    if len(stages) > 1:
        main_stage(*stages[0])
        far_half(0)
        main_stage(*stages[1])
        done = groups * stages[2][0]

        def begin(plane, carry):
            acc[plane] = (terms(plane, 0, done) + flag[...]).reshape(acc.shape[1:])
            return carry

        lax.fori_loop(0, n_col, begin, 0)
        far_half(1)
        main_stage(*stages[2])
    else:
        done = 0
        far_half(0)
        far_half(1)
        main_stage(*stages[0])

    home = [2, 1, 3, 0]
    S0 = M0 + 8
    spots = [(xp, (y * 2 + 1 - x)), (yp, ((1 - y) * 2 + x)), (dp, ((1 - y) * 2 + 1 - x))]
    order = [2, 0, 1]

    def pair_up(t):
        arrive(S0 + t, pairb.at[t])
        tot[t] = acc[(c + home[t]) % n_col, core] + pairb[t]
        for k in order:
            peer, there = spots[k]
            start(S0 + 4 + t * 3 + k, tot.at[t, there], inb.at[t, k], peer)

    def plane_sum(t):
        total = tot[t, chip]
        for k in range(3):
            arrive(S0 + 4 + t * 3 + k, inb.at[t, k])
            total = total + inb[t, k]
        return total

    for t in range(n_col):
        plane = (c + home[t]) % n_col
        part = terms(plane, done, edges).reshape(acc.shape[1:])
        acc[plane] = acc[plane] + part if done else part
        start(S0 + t, acc.at[plane, 1 - core], pairb.at[t], mate)
        if t:
            pair_up(t - 1)
    pair_up(n_col - 1)
    Z0 = S0 + 4 + n_col * 3
    for t in range(n_col - 1):
        zs[t] = plane_sum(t)
        start(Z0 + t, zs.at[t], zin.at[t], (r, (c + home[t]) % n_col))
    full = jnp.concatenate([lossp[i * groups : (i + 1) * groups] for i in range(group // LANE)], 1)
    high = full.astype(BF16).astype(F32)
    mid = (full - high).astype(BF16).astype(F32)
    low = full - high - mid
    shares = jnp.concatenate([high, mid, low, jnp.zeros_like(low)], 0).astype(BF16)
    which = lax.broadcasted_iota(jnp.int32, (groups, group), 0)

    def restore(g, carry):
        got = jnp.dot(shares, turn(g), preferred_element_type=F32)
        whole = got[:groups] + got[groups : 2 * groups] + got[2 * groups : 3 * groups]
        return jnp.where(which == g, whole, carry)

    back = lax.fori_loop(0, groups, restore, jnp.zeros((groups, group), F32))
    for g in range(groups):
        for i in range(group // LANE):
            at = g * (group // LANE) + i
            loss[at : at + 1, :] = back[g : g + 1, i * LANE : (i + 1) * LANE]
    total = plane_sum(n_col - 1)
    for t in range(n_col - 1):
        arrive(Z0 + t, zin.at[t])
        total = total + zin[t]
    grad[0] = total[:, :dim]
    grad[1] = total[:, WIDE : WIDE + dim]
    late[...] = total[:8, WIDE - LANE : WIDE]

    for cond, move in started:
        if cond is None:
            move.wait_send()
        else:
            pl.when(cond)(move.wait_send)


def step_call(n_row, n_col, fast, ent, rel, src_index, dst_index, rel_index, neg_block):
    edges, groups = src_index.shape[0], neg_block.shape[0]
    group = edges // groups
    parts, dim, count = ent.shape
    n_rel = rel.shape[2]
    span = n_rel // (n_row * n_col)
    chips = n_row // 2
    stages = ((0, 256), (256, 128), (384, 128)) if fast else ((0, group),)
    flat = lambda a: a.reshape(1, edges)
    smem = pl.BlockSpec(memory_space=pltpu.SMEM)
    vmem = pl.BlockSpec(memory_space=pltpu.VMEM)
    hbm = pl.BlockSpec(memory_space=pltpu.HBM)
    dma = pltpu.SemaphoreType.DMA
    copies = 4 * (n_col - 1) + 14 + 4 + n_col * 3 + n_col - 1
    return pl.pallas_call(
        functools.partial(step_kernel, n_col, group, stages),
        name="step" if fast else "step_late",
        out_shape=(
            jax.ShapeDtypeStruct((edges // LANE, LANE), F32),
            jax.ShapeDtypeStruct((parts, span, dim), F32),
            jax.ShapeDtypeStruct((8, LANE), F32),
        ),
        in_specs=[smem, vmem, vmem, vmem, hbm, hbm],
        out_specs=(vmem, vmem, vmem),
        scratch_shapes=[
            pltpu.VMEM((n_col * count // NEGB, parts, dim, NEGB), BF16),
            pltpu.VMEM((n_row * count // NEGB, parts, dim, NEGB), BF16),
            pltpu.VMEM(rel.shape, BF16),
            pltpu.VMEM((n_col * count, 4, LANE), F32),
            pltpu.VMEM((n_row * count, 4, LANE), F32),
            pltpu.VMEM((n_rel, 4, LANE), F32),
            pltpu.VMEM((group * 4, LANE), F32),
            pltpu.VMEM((edges, 2 * WIDE), BF16),
            pltpu.VMEM((edges, 2 * WIDE), BF16),
            pltpu.VMEM((parts, group, dim), BF16),
            pltpu.VMEM((group, LANE), F32),
            pltpu.VMEM((1, edges), jnp.int32),
            pltpu.VMEM((groups, group), jnp.int32),
            pltpu.VMEM((6 * groups, group), F32),
            pltpu.VMEM((3, groups, group), jnp.int32),
            pltpu.SMEM((3, groups, group), jnp.int32),
            pltpu.VMEM((edges // LANE, LANE), F32),
            pltpu.VMEM((1, 2 * WIDE), F32),
            pltpu.VMEM((n_col, 2, chips, span, 2 * WIDE), F32),
            pltpu.VMEM((n_col, chips, span, 2 * WIDE), F32),
            pltpu.VMEM((n_col, chips, span, 2 * WIDE), F32),
            pltpu.VMEM((n_col, 3, span, 2 * WIDE), F32),
            pltpu.VMEM((n_col - 1, span, 2 * WIDE), F32),
            pltpu.VMEM((n_col - 1, span, 2 * WIDE), F32),
            dma((4,)), dma((copies,)), dma((copies,)),
        ],
        compiler_params=pltpu.CompilerParams(
            collective_id=0 if fast else 1, has_side_effects=True, vmem_limit_bytes=67043328
        ),
    )(neg_block, flat(src_index), flat(dst_index), flat(rel_index), ent, rel)


def body(n_row, n_col, entities, relations, src_index, dst_index, rel_index, neg_block):
    dim = entities.shape[2]
    count = entities.shape[1]
    args = (entities, relations, src_index, dst_index, rel_index, neg_block)
    fits = LANE < dim < WIDE and (n_row + n_col) * count * 4 * LANE * 4 <= 26 * 2**20
    if n_row != 8 or n_col != 4 or count != 2 * NEGB or not fits:
        return wide_body(*args)
    if src_index.shape[0] != 8 * neg_block.shape[0] * 64 or neg_block.shape[0] != 8:
        return wide_body(*args)
    flip = lambda a: jnp.transpose(a, (0, 2, 1))
    whole = (flip(entities), flip(relations), src_index, dst_index, rel_index, neg_block)
    edge_loss, grad, late = step_call(n_row, n_col, True, *whole)
    edge_loss, grad = lax.cond(
        late[0, LANE - 1] > 0.0,
        lambda: tuple(step_call(n_row, n_col, False, *whole)[:2]),
        lambda: (edge_loss, grad),
    )
    return edge_loss.reshape(-1), grad


def bucket_terms(picked_src, picked_dst, negatives, relations, rel_ids):
    onehot = (rel_ids[:, None] == jnp.arange(relations.shape[1], dtype=jnp.int32)[None, :]).astype(
        jnp.bfloat16
    )
    rel_re = jnp.dot(onehot, relations[0], preferred_element_type=jnp.float32)
    rel_im = jnp.dot(onehot, relations[1], preferred_element_type=jnp.float32)
    src_re = picked_src[0].astype(jnp.float32)
    src_im = picked_src[1].astype(jnp.float32)
    dst_re = picked_dst[0].astype(jnp.float32)
    dst_im = picked_dst[1].astype(jnp.float32)
    query_re = src_re * rel_re - src_im * rel_im
    query_im = src_re * rel_im + src_im * rel_re
    pos_score = jnp.sum(query_re * dst_re, 1) + jnp.sum(query_im * dst_im, 1)
    groups = negatives.shape[1]
    dim = query_re.shape[1]
    qre_b = query_re.astype(jnp.bfloat16).reshape(groups, -1, dim)
    qim_b = query_im.astype(jnp.bfloat16).reshape(groups, -1, dim)
    neg_score = jnp.einsum(
        "kcd,knd->kcn", qre_b, negatives[0], preferred_element_type=jnp.float32
    ) + jnp.einsum("kcd,knd->kcn", qim_b, negatives[1], preferred_element_type=jnp.float32)
    edge_loss = jax.nn.softplus(-pos_score) + jnp.mean(jax.nn.softplus(neg_score), -1).reshape(-1)
    weights = (jax.nn.sigmoid(neg_score) / NEGB).astype(jnp.bfloat16)
    gneg_re = jnp.einsum(
        "kcn,knd->kcd", weights, negatives[0], preferred_element_type=jnp.float32
    ).reshape(-1, dim)
    gneg_im = jnp.einsum(
        "kcn,knd->kcd", weights, negatives[1], preferred_element_type=jnp.float32
    ).reshape(-1, dim)
    pull = jax.nn.sigmoid(-pos_score)[:, None]
    grad_re = gneg_re - pull * dst_re
    grad_im = gneg_im - pull * dst_im
    term_re = (grad_re * src_re + grad_im * src_im).astype(jnp.bfloat16)
    term_im = (grad_im * src_re - grad_re * src_im).astype(jnp.bfloat16)
    dims = (((0,), (0,)), ((), ()))
    rel_grad = jnp.stack(
        [
            lax.dot_general(onehot, term_re, dims, preferred_element_type=jnp.float32),
            lax.dot_general(onehot, term_im, dims, preferred_element_type=jnp.float32),
        ],
        0,
    )
    return (edge_loss, rel_grad)


def wide_body(entities, relations, src_index, dst_index, rel_index, neg_block):
    dim = entities.shape[2]
    source_rows = lax.all_gather(entities, "col", axis=1, tiled=True)
    picked_src = jnp.take(source_rows, src_index, axis=1)
    target_rows = lax.all_gather(entities, "row", axis=1, tiled=True)
    picked_dst = jnp.take(target_rows, dst_index, axis=1)
    negatives = jnp.take(target_rows.reshape(2, -1, NEGB, dim), neg_block, axis=1)
    edge_loss, rel_grad = bucket_terms(picked_src, picked_dst, negatives, relations, rel_index)
    row_share = lax.psum_scatter(rel_grad, "row", scatter_dimension=1, tiled=True)
    grad_share = lax.psum_scatter(row_share, "col", scatter_dimension=1, tiled=True)
    return (edge_loss, grad_share)


def solution(mesh):
    placed = (
        P(None, ("row", "col"), None),
        P(),
        P(("row", "col")),
        P(("row", "col")),
        P(("row", "col")),
        P(("row", "col")),
    )
    return jax.shard_map(
        functools.partial(body, mesh.shape["row"], mesh.shape["col"]),
        mesh=mesh,
        in_specs=placed,
        out_specs=(P(("row", "col")), P(None, ("row", "col"), None)),
        check_vma=False,
    )
```

```python
import functools

import jax
import jax.numpy as jnp
from jax import lax
from jax.experimental import pallas as pl
from jax.experimental.pallas import tpu as pltpu
from jax.sharding import PartitionSpec as P

NEGB = 512
LANE = 128
WIDE = 256
MESH = pl.DeviceIdType.MESH
F32 = jnp.float32
BF16 = jnp.bfloat16
PICKS = 32
QROWS = 32


def log1p_small(u):
    return jnp.where(u < 2.0**-9, u - 0.5 * u * u, jnp.log(1.0 + u))


def step_kernel(
    n_col, group, stages, neg_i, src_row, dst_row, rel_row, ent, rel, loss, grad, late,
    srcb, dstb, relb, s_tab, o_tab, w_tab, gs, go, gw, qb, dots, key, spot, moved, order_v, order_t, order_s, lossp, flag,
    acc, pairb, tot, inb, zs, zin, loc_sem, send_sem, recv_sem,
):
    r, c = lax.axis_index("row"), lax.axis_index("col")
    chip, core = r // 2, r % 2
    y, x = chip // 2, chip % 2
    row_of = lambda yy, xx, k: (yy * 2 + xx) * 2 + k
    xr, yr, dr = row_of(y, 1 - x, core), row_of(1 - y, x, core), row_of(1 - y, 1 - x, core)
    mr, mx, my, md = (row_of(yy, xx, 1 - core) for yy, xx in ((y, x), (y, 1 - x), (1 - y, x), (1 - y, 1 - x)))
    mate, xp, yp, dp = (mr, c), (xr, c), (yr, c), (dr, c)
    dim, count = ent.shape[1], ent.shape[2]
    n_rel = rel.shape[2]
    groups = neg_i.shape[0]
    edges = gw.shape[0]
    per = count // NEGB
    rest = dim - LANE

    barrier = pltpu.get_barrier_semaphore()
    peers = [mate, xp, yp, dp] + [(r, (c + b) % n_col) for b in range(1, n_col)]
    for peer in peers:
        pl.semaphore_signal(barrier, inc=1, device_id=peer, device_id_type=MESH)
    pl.semaphore_wait(barrier, len(peers))

    started = []

    def copy(k, src, dst, peer):
        return pltpu.make_async_remote_copy(
            src_ref=src, dst_ref=dst, send_sem=send_sem.at[k], recv_sem=recv_sem.at[k],
            device_id=peer, device_id_type=MESH,
        )

    def start(k, src, dst, peer):
        move = copy(k, src, dst, peer)
        move.start()
        started.append((None, move))

    def arrive(k, dst):
        copy(k, dst, dst, mate).wait_recv()

    own = lambda p: ent.at[:, :, p * NEGB : (p + 1) * NEGB]
    inside = lambda v: jnp.logical_and(v >= 0, v < n_col)

    def line_id(way, age, part):
        return ((0 if way > 0 else n_col - 1) + age) * 2 + part

    def line_send(way, age, part):
        shard = c - way * age
        cond = jnp.logical_and(inside(c + way), inside(shard))
        src = own(part) if age == 0 else srcb.at[shard * per + part]
        move = copy(line_id(way, age, part), src, srcb.at[shard * per + part], (r, c + way))

        @pl.when(cond)
        def _():
            move.start()

        started.append((cond, move))

    def line_wait(way, age, part):
        shard = c - way * (age + 1)

        @pl.when(inside(shard))
        def _():
            arrive(line_id(way, age, part), srcb.at[shard * per + part])

    base = 4 * (n_col - 1)
    X0, X1, Y0, Y1, XD, YD, M0 = (base + k for k in range(7))
    at_dst = lambda i, p: dstb.at[i * per + p]

    line_send(1, 0, 0)
    line_send(-1, 0, 0)
    start(X0, own(0), at_dst(r, 0), xp)
    start(Y1, own(1), at_dst(r, 1), yp)
    local_rel = pltpu.make_async_copy(rel, relb, loc_sem.at[0])
    local_ent = [pltpu.make_async_copy(own(p), at_dst(r, p), loc_sem.at[1 + p]) for p in range(per)]
    local_rel.start()
    for move in local_ent:
        move.start()
    line_send(1, 0, 1)
    line_send(-1, 0, 1)
    start(X1, own(1), at_dst(r, 1), xp)
    start(Y0, own(0), at_dst(r, 0), yp)
    start(M0, own(0), at_dst(r, 0), mate)
    start(M0 + 1, own(1), at_dst(r, 1), mate)

    def fill(read, targets):
        def step(j, carry):
            col = pl.multiple_of(j * LANE, LANE)
            for part in range(2):
                low = read(part, slice(0, LANE), col).astype(F32).T
                high = read(part, slice(LANE, dim), col).astype(F32)
                high = jnp.concatenate([high, jnp.zeros((LANE - rest, LANE), F32)], 0).T
                for table, first, _ in targets:
                    flat = table.reshape(table.shape[0] * 4, LANE)
                    at = first + col * 4 + part * 2
                    flat[pl.ds(at, LANE, stride=4), :] = low
                    flat[pl.ds(at + 1, LANE, stride=4), :] = high
            return carry

        lax.fori_loop(0, targets[0][2] // LANE, step, 0)

    def fill_half(buf, half, *tables):
        fill(
            lambda p, rows, col: buf[half, p, rows, pl.ds(col, LANE)],
            [(table, shard * (NEGB * 4), NEGB) for table, shard in tables],
        )

    def fill_dst(shard):
        for p in range(per):
            half = shard * per + p
            fill_half(dstb, half, (o_tab, half))

    def fill_src(shard):
        @pl.when(inside(shard))
        def _():
            for p in range(per):
                half = shard * per + p
                fill_half(srcb, half, (s_tab, half))

    def pick(table, kind, g, low, rows):
        top = table.shape[0] - 1
        keep = (lambda v: v & top) if top & (top + 1) == 0 else (lambda v: jnp.clip(v, 0, top))
        start_row = kind * (edges // LANE) + low // LANE * groups + g

        def step(i, carry):
            row = start_row + i * groups
            for part in range(0, LANE, PICKS):
                got = [table[keep(order_s[row, part + u])] for u in range(PICKS)]
                for u in range(PICKS):
                    gs[pl.ds(pl.multiple_of((i * LANE + part + u) * 4, 4), 4), :] = got[u]
            return carry

        lax.fori_loop(0, rows // LANE, step, 0)

    def pick_all(table, kind, out):
        for low, rows in stages:
            def one(g, carry, low=low, rows=rows):
                pick(table, kind, g, low, rows)

                def pack(i, inner):
                    row = pl.multiple_of(i * QROWS, QROWS)
                    at = pl.ds(pl.multiple_of(groups * low + g * rows + row, QROWS), QROWS)
                    for k in range(4):
                        out[at, k * LANE : (k + 1) * LANE] = gs[pl.ds(row * 4 + k, QROWS, stride=4), :].astype(BF16)
                    return inner

                lax.fori_loop(0, rows // QROWS, pack, 0)
                return carry

            lax.fori_loop(0, groups, one, 0)

    span = n_rel // (8 * n_col)
    for g in range(groups):
        cut = slice(g * group, (g + 1) * group)
        for kind, ref in enumerate((src_row, dst_row, rel_row)):
            order_v[kind, g : g + 1, :] = ref[:, cut]
    halves = lax.div(order_v[0], NEGB)
    far = jnp.abs(lax.div(halves, per) - c) == n_col - 1
    last = jnp.logical_and(far, lax.rem(halves, per) == per - 1)
    early = jnp.where(far, 0.0, 1.0)
    middle = jnp.where(last, 0.0, 1.0) - early
    lane_id = lax.broadcasted_iota(jnp.int32, (groups, group), 1).astype(F32)
    before = lax.broadcasted_iota(jnp.int32, (group, group), 0) < lax.broadcasted_iota(jnp.int32, (group, group), 1)
    ahead = jnp.dot(
        jnp.concatenate([early, middle], 0).astype(BF16), jnp.where(before, 1.0, 0.0).astype(BF16),
        preferred_element_type=F32,
    )
    ahead0, ahead1 = ahead[:groups], ahead[groups:]
    n_early = jnp.sum(early, 1, keepdims=True)
    n_middle = jnp.sum(middle, 1, keepdims=True)
    place = jnp.where(
        far, jnp.where(last, n_early + n_middle + lane_id - ahead0 - ahead1, n_early + ahead1), ahead0
    )
    spot[...] = place.astype(jnp.int32)
    if len(stages) > 1:
        short = jnp.maximum(
            jnp.where(n_early < float(stages[1][0]), 1.0, 0.0),
            jnp.where(n_early + n_middle < float(stages[2][0]), 1.0, 0.0),
        )
        lanes = lax.broadcasted_iota(jnp.int32, (1, 2 * WIDE), 1)
        flag[...] = jnp.where(lanes == WIDE - 1, jnp.sum(short, 0, keepdims=True), 0.0)
    else:
        flag[...] = jnp.zeros_like(flag)

    def turn(g):
        ids = lax.broadcasted_iota(jnp.int32, (group, group), 0)
        return jnp.where(ids == spot[pl.ds(g, 1), :], 1.0, 0.0).astype(BF16)

    split = []
    for kind in range(3):
        split += [lax.div(order_v[kind], LANE), lax.rem(order_v[kind], LANE)]
    moved[...] = jnp.concatenate(split, 0).astype(F32)
    pieces = moved[...].astype(BF16)
    mine = lax.rem(lax.broadcasted_iota(jnp.int32, (6 * groups, group), 0), groups)
    nt = (((1,), (1,)), ((), ()))

    def reorder(g, carry):
        got = lax.dot_general(pieces, turn(g), nt, preferred_element_type=F32)
        moved[...] = jnp.where(mine == g, got, moved[...])
        return carry

    lax.fori_loop(0, groups, reorder, 0)
    for kind in range(3):
        at = kind * 2 * groups
        order_v[kind] = (moved[at : at + groups] * LANE + moved[at + groups : at + 2 * groups]).astype(jnp.int32)
    blocks = group // LANE
    for kind in range(3):
        for i in range(blocks):
            at = (kind * blocks + i) * groups
            order_t[at : at + groups, :] = order_v[kind, :, i * LANE : (i + 1) * LANE]
    to_scalar = pltpu.make_async_copy(order_t, order_s, loc_sem.at[3])
    to_scalar.start()
    rel_ids = order_v[2]
    row_part = lax.div(rel_ids, n_col * span)
    keys = (
        lax.rem(lax.div(rel_ids, span), n_col) * (8 * span)
        + lax.rem(row_part, 2) * (4 * span) + lax.div(row_part, 2) * span + lax.rem(rel_ids, span)
    )
    for low, rows in stages:
        for g in range(groups):
            at = groups * low + g * rows
            key[:, at : at + rows] = keys[g : g + 1, low : low + rows]
    to_scalar.wait()

    local_rel.wait()
    fill(lambda p, rows, col: relb[p, rows, pl.ds(col, LANE)], [(w_tab, 0, n_rel)])
    pick_all(w_tab, 2, gw)
    for move in local_ent:
        move.wait()
    for p in range(per):
        fill_half(dstb, r * per + p, (o_tab, r * per + p), (s_tab, c * per + p))

    arrive(X0, at_dst(xr, 0))
    start(YD, at_dst(xr, 0), at_dst(xr, 0), yp)
    arrive(Y1, at_dst(yr, 1))
    start(XD, at_dst(yr, 1), at_dst(yr, 1), xp)
    for way in (1, -1):
        line_wait(way, 0, 0)
        line_send(way, 1, 0)
    start(M0 + 2, at_dst(xr, 0), at_dst(xr, 0), mate)
    start(M0 + 3, at_dst(yr, 1), at_dst(yr, 1), mate)
    arrive(M0, at_dst(mr, 0))
    arrive(M0 + 1, at_dst(mr, 1))
    fill_dst(mr)

    arrive(X1, at_dst(xr, 1))
    start(M0 + 4, at_dst(xr, 1), at_dst(xr, 1), mate)
    arrive(Y0, at_dst(yr, 0))
    start(M0 + 5, at_dst(yr, 0), at_dst(yr, 0), mate)
    for way in (1, -1):
        line_wait(way, 0, 1)
        line_send(way, 1, 1)
    fill_dst(xr)
    fill_dst(yr)
    fill_src(c - 1)
    fill_src(c + 1)
    arrive(M0 + 2, at_dst(mx, 0))
    arrive(M0 + 4, at_dst(mx, 1))
    fill_dst(mx)
    arrive(M0 + 3, at_dst(my, 1))
    arrive(M0 + 5, at_dst(my, 0))
    fill_dst(my)

    arrive(YD, at_dst(dr, 0))
    start(M0 + 6, at_dst(dr, 0), at_dst(dr, 0), mate)
    arrive(XD, at_dst(dr, 1))
    start(M0 + 7, at_dst(dr, 1), at_dst(dr, 1), mate)
    for way in (1, -1):
        line_wait(way, 1, 0)
        line_send(way, 2, 0)
    fill_dst(dr)
    arrive(M0 + 6, at_dst(md, 0))
    arrive(M0 + 7, at_dst(md, 1))
    fill_dst(md)
    pick_all(o_tab, 1, go)

    for way in (1, -1):
        line_wait(way, 1, 1)
        line_send(way, 2, 1)
    fill_src(c - 2)
    fill_src(c + 2)
    eye = lax.broadcasted_iota(jnp.int32, (LANE, LANE), 0) == lax.broadcasted_iota(jnp.int32, (LANE, LANE), 1)
    cuts = ((0, LANE), (LANE, dim))

    def main_stage(low_row, size):
        def one_group(g, carry):
            pick(s_tab, 0, g, low_row, size)
            first = groups * low_row + g * size

            def query(i, inner):
                row = pl.multiple_of(i * QROWS, QROWS)
                rows = pl.ds(pl.multiple_of(first + row, QROWS), QROWS)
                score = None
                for half, (low, high) in enumerate(cuts):
                    near = lambda p: gs[pl.ds(row * 4 + p * 2 + half, QROWS, stride=4), :]
                    dense = lambda ref, p: ref[rows, p * WIDE + half * LANE : p * WIDE + (half + 1) * LANE].astype(F32)
                    sr, si, wr, wi = near(0), near(1), dense(gw, 0), dense(gw, 1)
                    qr = sr * wr - si * wi
                    qi = sr * wi + si * wr
                    add = qr * dense(go, 0) + qi * dense(go, 1)
                    score = add if score is None else score + add
                    qb[0, pl.ds(row, QROWS), low:high] = qr[:, : high - low].astype(BF16)
                    qb[1, pl.ds(row, QROWS), low:high] = qi[:, : high - low].astype(BF16)
                dots[pl.ds(row, QROWS), :] = score
                return inner

            lax.fori_loop(0, size // QROWS, query, 0)
            b = neg_i[g]
            near = lambda p: dstb[b, p]
            score = jnp.dot(qb[0, :size], near(0), preferred_element_type=F32)
            score = score + jnp.dot(qb[1, :size], near(1), preferred_element_type=F32)
            small = jnp.exp(-jnp.abs(score))
            soft = jnp.maximum(score, 0.0) + log1p_small(small)
            ratio = 1.0 / (1.0 + small)
            weight = jnp.where(score >= 0.0, ratio, small * ratio).astype(BF16)
            p = jnp.sum(dots[:size], 1, keepdims=True)
            p_small = jnp.exp(-jnp.abs(p))
            value = jnp.maximum(-p, 0.0) + log1p_small(p_small) + jnp.sum(soft, 1, keepdims=True) * (1.0 / NEGB)
            pull = jnp.where(p >= 0.0, p_small, 1.0) / (1.0 + p_small)
            for i in range(size // LANE):
                piece = value[i * LANE : (i + 1) * LANE]
                lossp[pl.ds((low_row // LANE + i) * groups + g, 1), :] = jnp.sum(jnp.where(eye, piece, 0.0), 0, keepdims=True)
            g_re = lax.dot_general(weight, near(0), nt, preferred_element_type=F32) * (1.0 / NEGB)
            g_im = lax.dot_general(weight, near(1), nt, preferred_element_type=F32) * (1.0 / NEGB)
            rows = pl.ds(pl.multiple_of(first, size), size)
            for half, (low, high) in enumerate(cuts):
                wide = high - low
                part = lambda q: gs[pl.ds(q * 2 + half, size, stride=4), :][:, :wide]
                lanes = lambda q: slice(q * WIDE + low, q * WIDE + high)
                d_re = g_re[:, low:high] - pull * go[rows, lanes(0)].astype(F32)
                d_im = g_im[:, low:high] - pull * go[rows, lanes(1)].astype(F32)
                s_re, s_im = part(0), part(1)
                gw[rows, lanes(0)] = (d_re * s_re + d_im * s_im).astype(BF16)
                gw[rows, lanes(1)] = (d_im * s_re - d_re * s_im).astype(BF16)
            return carry

        lax.fori_loop(0, groups, one_group, 0)

    tile = 8 * span

    def far_half(p):
        for way in (1, -1):
            line_wait(way, n_col - 2, p)
            shard = c - way * (n_col - 1)

            @pl.when(inside(shard))
            def _():
                fill_half(srcb, shard * per + p, (s_tab, shard * per + p))

    def terms(plane, low, high):
        ids = lax.broadcasted_iota(jnp.int32, (tile, high - low), 0) + plane * tile
        hot = jnp.where(ids == key[:, low:high], 1.0, 0.0).astype(BF16)
        return jnp.dot(hot, gw[low:high], preferred_element_type=F32)

    if len(stages) > 1:
        main_stage(*stages[0])
        far_half(0)
        main_stage(*stages[1])
        done = groups * stages[2][0]

        def begin(plane, carry):
            acc[plane] = (terms(plane, 0, done) + flag[...]).reshape(acc.shape[1:])
            return carry

        lax.fori_loop(0, n_col, begin, 0)
        far_half(1)
        main_stage(*stages[2])
    else:
        done = 0
        far_half(0)
        far_half(1)
        main_stage(*stages[0])

    home = [2, 1, 3, 0]
    S0 = M0 + 8
    spots = [(xp, (y * 2 + 1 - x)), (yp, ((1 - y) * 2 + x)), (dp, ((1 - y) * 2 + 1 - x))]
    order = [2, 0, 1]

    def pair_up(t):
        arrive(S0 + t, pairb.at[t])
        tot[t] = acc[(c + home[t]) % n_col, core] + pairb[t]
        for k in order:
            peer, there = spots[k]
            start(S0 + 4 + t * 3 + k, tot.at[t, there], inb.at[t, k], peer)

    def plane_sum(t):
        total = tot[t, chip]
        for k in range(3):
            arrive(S0 + 4 + t * 3 + k, inb.at[t, k])
            total = total + inb[t, k]
        return total

    for t in range(n_col):
        plane = (c + home[t]) % n_col
        part = terms(plane, done, edges).reshape(acc.shape[1:])
        acc[plane] = acc[plane] + part if done else part
        start(S0 + t, acc.at[plane, 1 - core], pairb.at[t], mate)
        if t:
            pair_up(t - 1)
    pair_up(n_col - 1)
    Z0 = S0 + 4 + n_col * 3
    for t in range(n_col - 1):
        zs[t] = plane_sum(t)
        start(Z0 + t, zs.at[t], zin.at[t], (r, (c + home[t]) % n_col))
    full = jnp.concatenate([lossp[i * groups : (i + 1) * groups] for i in range(group // LANE)], 1)
    high = full.astype(BF16).astype(F32)
    mid = (full - high).astype(BF16).astype(F32)
    low = full - high - mid
    shares = jnp.concatenate([high, mid, low, jnp.zeros_like(low)], 0).astype(BF16)
    which = lax.broadcasted_iota(jnp.int32, (groups, group), 0)

    def restore(g, carry):
        got = jnp.dot(shares, turn(g), preferred_element_type=F32)
        whole = got[:groups] + got[groups : 2 * groups] + got[2 * groups : 3 * groups]
        return jnp.where(which == g, whole, carry)

    back = lax.fori_loop(0, groups, restore, jnp.zeros((groups, group), F32))
    for g in range(groups):
        for i in range(group // LANE):
            at = g * (group // LANE) + i
            loss[at : at + 1, :] = back[g : g + 1, i * LANE : (i + 1) * LANE]
    total = plane_sum(n_col - 1)
    for t in range(n_col - 1):
        arrive(Z0 + t, zin.at[t])
        total = total + zin[t]
    grad[0] = total[:, :dim]
    grad[1] = total[:, WIDE : WIDE + dim]
    late[...] = total[:8, WIDE - LANE : WIDE]

    for cond, move in started:
        if cond is None:
            move.wait_send()
        else:
            pl.when(cond)(move.wait_send)


def step_call(n_row, n_col, fast, ent, rel, src_index, dst_index, rel_index, neg_block):
    edges, groups = src_index.shape[0], neg_block.shape[0]
    group = edges // groups
    parts, dim, count = ent.shape
    n_rel = rel.shape[2]
    span = n_rel // (n_row * n_col)
    chips = n_row // 2
    stages = ((0, 256), (256, 128), (384, 128)) if fast else ((0, group),)
    flat = lambda a: a.reshape(1, edges)
    smem = pl.BlockSpec(memory_space=pltpu.SMEM)
    vmem = pl.BlockSpec(memory_space=pltpu.VMEM)
    hbm = pl.BlockSpec(memory_space=pltpu.HBM)
    dma = pltpu.SemaphoreType.DMA
    copies = 4 * (n_col - 1) + 14 + 4 + n_col * 3 + n_col - 1
    return pl.pallas_call(
        functools.partial(step_kernel, n_col, group, stages),
        name="step" if fast else "step_late",
        out_shape=(
            jax.ShapeDtypeStruct((edges // LANE, LANE), F32),
            jax.ShapeDtypeStruct((parts, span, dim), F32),
            jax.ShapeDtypeStruct((8, LANE), F32),
        ),
        in_specs=[smem, vmem, vmem, vmem, hbm, hbm],
        out_specs=(vmem, vmem, vmem),
        scratch_shapes=[
            pltpu.VMEM((n_col * count // NEGB, parts, dim, NEGB), BF16),
            pltpu.VMEM((n_row * count // NEGB, parts, dim, NEGB), BF16),
            pltpu.VMEM(rel.shape, BF16),
            pltpu.VMEM((n_col * count, 4, LANE), F32),
            pltpu.VMEM((n_row * count, 4, LANE), F32),
            pltpu.VMEM((n_rel, 4, LANE), F32),
            pltpu.VMEM((group * 4, LANE), F32),
            pltpu.VMEM((edges, 2 * WIDE), BF16),
            pltpu.VMEM((edges, 2 * WIDE), BF16),
            pltpu.VMEM((parts, group, dim), BF16),
            pltpu.VMEM((group, LANE), F32),
            pltpu.VMEM((1, edges), jnp.int32),
            pltpu.VMEM((groups, group), jnp.int32),
            pltpu.VMEM((6 * groups, group), F32),
            pltpu.VMEM((3, groups, group), jnp.int32),
            pltpu.VMEM((3 * edges // LANE, LANE), jnp.int32),
            pltpu.SMEM((3 * edges // LANE, LANE), jnp.int32),
            pltpu.VMEM((edges // LANE, LANE), F32),
            pltpu.VMEM((1, 2 * WIDE), F32),
            pltpu.VMEM((n_col, 2, chips, span, 2 * WIDE), F32),
            pltpu.VMEM((n_col, chips, span, 2 * WIDE), F32),
            pltpu.VMEM((n_col, chips, span, 2 * WIDE), F32),
            pltpu.VMEM((n_col, 3, span, 2 * WIDE), F32),
            pltpu.VMEM((n_col - 1, span, 2 * WIDE), F32),
            pltpu.VMEM((n_col - 1, span, 2 * WIDE), F32),
            dma((4,)), dma((copies,)), dma((copies,)),
        ],
        compiler_params=pltpu.CompilerParams(
            collective_id=0 if fast else 1, has_side_effects=True, vmem_limit_bytes=67043328
        ),
    )(neg_block, flat(src_index), flat(dst_index), flat(rel_index), ent, rel)


def body(n_row, n_col, entities, relations, src_index, dst_index, rel_index, neg_block):
    dim = entities.shape[2]
    count = entities.shape[1]
    args = (entities, relations, src_index, dst_index, rel_index, neg_block)
    fits = LANE < dim < WIDE and (n_row + n_col) * count * 4 * LANE * 4 <= 26 * 2**20
    if n_row != 8 or n_col != 4 or count != 2 * NEGB or not fits:
        return wide_body(*args)
    if src_index.shape[0] != 8 * neg_block.shape[0] * 64 or neg_block.shape[0] != 8:
        return wide_body(*args)
    flip = lambda a: jnp.transpose(a, (0, 2, 1))
    whole = (flip(entities), flip(relations), src_index, dst_index, rel_index, neg_block)
    edge_loss, grad, late = step_call(n_row, n_col, True, *whole)
    edge_loss, grad = lax.cond(
        late[0, LANE - 1] > 0.0,
        lambda: tuple(step_call(n_row, n_col, False, *whole)[:2]),
        lambda: (edge_loss, grad),
    )
    return edge_loss.reshape(-1), grad


def bucket_terms(picked_src, picked_dst, negatives, relations, rel_ids):
    onehot = (rel_ids[:, None] == jnp.arange(relations.shape[1], dtype=jnp.int32)[None, :]).astype(
        jnp.bfloat16
    )
    rel_re = jnp.dot(onehot, relations[0], preferred_element_type=jnp.float32)
    rel_im = jnp.dot(onehot, relations[1], preferred_element_type=jnp.float32)
    src_re = picked_src[0].astype(jnp.float32)
    src_im = picked_src[1].astype(jnp.float32)
    dst_re = picked_dst[0].astype(jnp.float32)
    dst_im = picked_dst[1].astype(jnp.float32)
    query_re = src_re * rel_re - src_im * rel_im
    query_im = src_re * rel_im + src_im * rel_re
    pos_score = jnp.sum(query_re * dst_re, 1) + jnp.sum(query_im * dst_im, 1)
    groups = negatives.shape[1]
    dim = query_re.shape[1]
    qre_b = query_re.astype(jnp.bfloat16).reshape(groups, -1, dim)
    qim_b = query_im.astype(jnp.bfloat16).reshape(groups, -1, dim)
    neg_score = jnp.einsum(
        "kcd,knd->kcn", qre_b, negatives[0], preferred_element_type=jnp.float32
    ) + jnp.einsum("kcd,knd->kcn", qim_b, negatives[1], preferred_element_type=jnp.float32)
    edge_loss = jax.nn.softplus(-pos_score) + jnp.mean(jax.nn.softplus(neg_score), -1).reshape(-1)
    weights = (jax.nn.sigmoid(neg_score) / NEGB).astype(jnp.bfloat16)
    gneg_re = jnp.einsum(
        "kcn,knd->kcd", weights, negatives[0], preferred_element_type=jnp.float32
    ).reshape(-1, dim)
    gneg_im = jnp.einsum(
        "kcn,knd->kcd", weights, negatives[1], preferred_element_type=jnp.float32
    ).reshape(-1, dim)
    pull = jax.nn.sigmoid(-pos_score)[:, None]
    grad_re = gneg_re - pull * dst_re
    grad_im = gneg_im - pull * dst_im
    term_re = (grad_re * src_re + grad_im * src_im).astype(jnp.bfloat16)
    term_im = (grad_im * src_re - grad_re * src_im).astype(jnp.bfloat16)
    dims = (((0,), (0,)), ((), ()))
    rel_grad = jnp.stack(
        [
            lax.dot_general(onehot, term_re, dims, preferred_element_type=jnp.float32),
            lax.dot_general(onehot, term_im, dims, preferred_element_type=jnp.float32),
        ],
        0,
    )
    return (edge_loss, rel_grad)


def wide_body(entities, relations, src_index, dst_index, rel_index, neg_block):
    dim = entities.shape[2]
    source_rows = lax.all_gather(entities, "col", axis=1, tiled=True)
    picked_src = jnp.take(source_rows, src_index, axis=1)
    target_rows = lax.all_gather(entities, "row", axis=1, tiled=True)
    picked_dst = jnp.take(target_rows, dst_index, axis=1)
    negatives = jnp.take(target_rows.reshape(2, -1, NEGB, dim), neg_block, axis=1)
    edge_loss, rel_grad = bucket_terms(picked_src, picked_dst, negatives, relations, rel_index)
    row_share = lax.psum_scatter(rel_grad, "row", scatter_dimension=1, tiled=True)
    grad_share = lax.psum_scatter(row_share, "col", scatter_dimension=1, tiled=True)
    return (edge_loss, grad_share)


def solution(mesh):
    placed = (
        P(None, ("row", "col"), None),
        P(),
        P(("row", "col")),
        P(("row", "col")),
        P(("row", "col")),
        P(("row", "col")),
    )
    return jax.shard_map(
        functools.partial(body, mesh.shape["row"], mesh.shape["col"]),
        mesh=mesh,
        in_specs=placed,
        out_specs=(P(("row", "col")), P(None, ("row", "col"), None)),
        check_vma=False,
    )
```

```python
import functools

import jax
import jax.numpy as jnp
from jax import lax
from jax.experimental import pallas as pl
from jax.experimental.pallas import tpu as pltpu
from jax.sharding import PartitionSpec as P

NEGB = 512
LANE = 128
WIDE = 256
MESH = pl.DeviceIdType.MESH
F32 = jnp.float32
BF16 = jnp.bfloat16
PICKS = 32
QROWS = 64
PROWS = 128


def log1p_small(u):
    return jnp.where(u < 2.0**-9, u - 0.5 * u * u, jnp.log(1.0 + u))


def step_kernel(
    n_col, group, stages, neg_i, src_row, dst_row, rel_row, ent, rel, loss, grad, late,
    srcb, dstb, relb, s_tab, o_tab, w_tab, gs, go, gw, qb, dots, key, spot, moved, order_v, order_t, order_s, lossp, flag,
    acc, pairb, tot, inb, zs, zin, loc_sem, send_sem, recv_sem,
):
    r, c = lax.axis_index("row"), lax.axis_index("col")
    chip, core = r // 2, r % 2
    y, x = chip // 2, chip % 2
    row_of = lambda yy, xx, k: (yy * 2 + xx) * 2 + k
    xr, yr, dr = row_of(y, 1 - x, core), row_of(1 - y, x, core), row_of(1 - y, 1 - x, core)
    mr, mx, my, md = (row_of(yy, xx, 1 - core) for yy, xx in ((y, x), (y, 1 - x), (1 - y, x), (1 - y, 1 - x)))
    mate, xp, yp, dp = (mr, c), (xr, c), (yr, c), (dr, c)
    dim, count = ent.shape[1], ent.shape[2]
    n_rel = rel.shape[2]
    groups = neg_i.shape[0]
    edges = gw.shape[0]
    per = count // NEGB
    rest = dim - LANE

    barrier = pltpu.get_barrier_semaphore()
    peers = [mate, xp, yp, dp] + [(r, (c + b) % n_col) for b in range(1, n_col)]
    for peer in peers:
        pl.semaphore_signal(barrier, inc=1, device_id=peer, device_id_type=MESH)
    pl.semaphore_wait(barrier, len(peers))

    started = []

    def copy(k, src, dst, peer):
        return pltpu.make_async_remote_copy(
            src_ref=src, dst_ref=dst, send_sem=send_sem.at[k], recv_sem=recv_sem.at[k],
            device_id=peer, device_id_type=MESH,
        )

    def start(k, src, dst, peer):
        move = copy(k, src, dst, peer)
        move.start()
        started.append((None, move))

    def arrive(k, dst):
        copy(k, dst, dst, mate).wait_recv()

    own = lambda p: ent.at[:, :, p * NEGB : (p + 1) * NEGB]
    inside = lambda v: jnp.logical_and(v >= 0, v < n_col)

    def line_id(way, age, part):
        return ((0 if way > 0 else n_col - 1) + age) * 2 + part

    def line_send(way, age, part):
        shard = c - way * age
        cond = jnp.logical_and(inside(c + way), inside(shard))
        src = own(part) if age == 0 else srcb.at[shard * per + part]
        move = copy(line_id(way, age, part), src, srcb.at[shard * per + part], (r, c + way))

        @pl.when(cond)
        def _():
            move.start()

        started.append((cond, move))

    def line_wait(way, age, part):
        shard = c - way * (age + 1)

        @pl.when(inside(shard))
        def _():
            arrive(line_id(way, age, part), srcb.at[shard * per + part])

    base = 4 * (n_col - 1)
    X0, X1, Y0, Y1, XD, YD, M0 = (base + k for k in range(7))
    at_dst = lambda i, p: dstb.at[i * per + p]

    line_send(1, 0, 0)
    line_send(-1, 0, 0)
    start(X0, own(0), at_dst(r, 0), xp)
    start(Y1, own(1), at_dst(r, 1), yp)
    local_rel = pltpu.make_async_copy(rel, relb, loc_sem.at[0])
    local_ent = [pltpu.make_async_copy(own(p), at_dst(r, p), loc_sem.at[1 + p]) for p in range(per)]
    local_rel.start()
    for move in local_ent:
        move.start()
    line_send(1, 0, 1)
    line_send(-1, 0, 1)
    start(X1, own(1), at_dst(r, 1), xp)
    start(Y0, own(0), at_dst(r, 0), yp)
    start(M0, own(0), at_dst(r, 0), mate)
    start(M0 + 1, own(1), at_dst(r, 1), mate)

    def fill(read, targets):
        def step(j, carry):
            for both in range(2):
                col = pl.multiple_of(j * (2 * LANE) + both * LANE, LANE)
                for part in range(2):
                    low = read(part, slice(0, LANE), col).astype(F32).T
                    high = read(part, slice(LANE, dim), col).astype(F32)
                    high = jnp.concatenate([high, jnp.zeros((LANE - rest, LANE), F32)], 0).T
                    for table, first, _ in targets:
                        flat = table.reshape(table.shape[0] * 4, LANE)
                        at = first + col * 4 + part * 2
                        flat[pl.ds(at, LANE, stride=4), :] = low
                        flat[pl.ds(at + 1, LANE, stride=4), :] = high
            return carry

        lax.fori_loop(0, targets[0][2] // (2 * LANE), step, 0)

    def fill_half(buf, half, *tables):
        fill(
            lambda p, rows, col: buf[half, p, rows, pl.ds(col, LANE)],
            [(table, shard * (NEGB * 4), NEGB) for table, shard in tables],
        )

    def fill_dst(shard):
        for p in range(per):
            half = shard * per + p
            fill_half(dstb, half, (o_tab, half))

    def fill_src(shard):
        @pl.when(inside(shard))
        def _():
            for p in range(per):
                half = shard * per + p
                fill_half(srcb, half, (s_tab, half))

    def pick(table, kind, g, low, rows):
        top = table.shape[0] - 1
        keep = (lambda v: v & top) if top & (top + 1) == 0 else (lambda v: jnp.clip(v, 0, top))
        start_row = kind * (edges // LANE) + low // LANE * groups + g

        def step(i, carry):
            row = start_row + i * groups
            for part in range(0, LANE, PICKS):
                got = [table[keep(order_s[row, part + u])] for u in range(PICKS)]
                for u in range(PICKS):
                    gs[pl.ds(pl.multiple_of((i * LANE + part + u) * 4, 4), 4), :] = got[u]
            return carry

        lax.fori_loop(0, rows // LANE, step, 0)

    def pick_all(table, kind, out):
        for low, rows in stages:
            def one(g, carry, low=low, rows=rows):
                pick(table, kind, g, low, rows)

                def pack(i, inner):
                    row = pl.multiple_of(i * PROWS, PROWS)
                    at = pl.ds(pl.multiple_of(groups * low + g * rows + row, PROWS), PROWS)
                    for k in range(4):
                        out[at, k * LANE : (k + 1) * LANE] = gs[pl.ds(row * 4 + k, PROWS, stride=4), :].astype(BF16)
                    return inner

                lax.fori_loop(0, rows // PROWS, pack, 0)
                return carry

            lax.fori_loop(0, groups, one, 0)

    span = n_rel // (8 * n_col)
    for g in range(groups):
        cut = slice(g * group, (g + 1) * group)
        for kind, ref in enumerate((src_row, dst_row, rel_row)):
            order_v[kind, g : g + 1, :] = ref[:, cut]
    halves = lax.div(order_v[0], NEGB)
    far = jnp.abs(lax.div(halves, per) - c) == n_col - 1
    last = jnp.logical_and(far, lax.rem(halves, per) == per - 1)
    early = jnp.where(far, 0.0, 1.0)
    middle = jnp.where(last, 0.0, 1.0) - early
    lane_id = lax.broadcasted_iota(jnp.int32, (groups, group), 1).astype(F32)
    before = lax.broadcasted_iota(jnp.int32, (group, group), 0) < lax.broadcasted_iota(jnp.int32, (group, group), 1)
    ahead = jnp.dot(
        jnp.concatenate([early, middle], 0).astype(BF16), jnp.where(before, 1.0, 0.0).astype(BF16),
        preferred_element_type=F32,
    )
    ahead0, ahead1 = ahead[:groups], ahead[groups:]
    n_early = jnp.sum(early, 1, keepdims=True)
    n_middle = jnp.sum(middle, 1, keepdims=True)
    place = jnp.where(
        far, jnp.where(last, n_early + n_middle + lane_id - ahead0 - ahead1, n_early + ahead1), ahead0
    )
    spot[...] = place.astype(jnp.int32)
    if len(stages) > 1:
        short = jnp.maximum(
            jnp.where(n_early < float(stages[1][0]), 1.0, 0.0),
            jnp.where(n_early + n_middle < float(stages[2][0]), 1.0, 0.0),
        )
        lanes = lax.broadcasted_iota(jnp.int32, (1, 2 * WIDE), 1)
        flag[...] = jnp.where(lanes == WIDE - 1, jnp.sum(short, 0, keepdims=True), 0.0)
    else:
        flag[...] = jnp.zeros_like(flag)

    def turn(g):
        ids = lax.broadcasted_iota(jnp.int32, (group, group), 0)
        return jnp.where(ids == spot[pl.ds(g, 1), :], 1.0, 0.0).astype(BF16)

    split = []
    for kind in range(3):
        split += [lax.div(order_v[kind], LANE), lax.rem(order_v[kind], LANE)]
    moved[...] = jnp.concatenate(split, 0).astype(F32)
    pieces = moved[...].astype(BF16)
    mine = lax.rem(lax.broadcasted_iota(jnp.int32, (6 * groups, group), 0), groups)
    nt = (((1,), (1,)), ((), ()))

    def reorder(g, carry):
        got = lax.dot_general(pieces, turn(g), nt, preferred_element_type=F32)
        moved[...] = jnp.where(mine == g, got, moved[...])
        return carry

    lax.fori_loop(0, groups, reorder, 0)
    for kind in range(3):
        at = kind * 2 * groups
        order_v[kind] = (moved[at : at + groups] * LANE + moved[at + groups : at + 2 * groups]).astype(jnp.int32)
    blocks = group // LANE
    for kind in range(3):
        for i in range(blocks):
            at = (kind * blocks + i) * groups
            order_t[at : at + groups, :] = order_v[kind, :, i * LANE : (i + 1) * LANE]
    to_scalar = pltpu.make_async_copy(order_t, order_s, loc_sem.at[3])
    to_scalar.start()
    rel_ids = order_v[2]
    row_part = lax.div(rel_ids, n_col * span)
    keys = (
        lax.rem(lax.div(rel_ids, span), n_col) * (8 * span)
        + lax.rem(row_part, 2) * (4 * span) + lax.div(row_part, 2) * span + lax.rem(rel_ids, span)
    )
    for low, rows in stages:
        for g in range(groups):
            at = groups * low + g * rows
            key[:, at : at + rows] = keys[g : g + 1, low : low + rows]
    to_scalar.wait()

    local_rel.wait()
    fill(lambda p, rows, col: relb[p, rows, pl.ds(col, LANE)], [(w_tab, 0, n_rel)])
    pick_all(w_tab, 2, gw)
    for move in local_ent:
        move.wait()
    for p in range(per):
        fill_half(dstb, r * per + p, (o_tab, r * per + p), (s_tab, c * per + p))

    arrive(X0, at_dst(xr, 0))
    start(YD, at_dst(xr, 0), at_dst(xr, 0), yp)
    arrive(Y1, at_dst(yr, 1))
    start(XD, at_dst(yr, 1), at_dst(yr, 1), xp)
    for way in (1, -1):
        line_wait(way, 0, 0)
        line_send(way, 1, 0)
    start(M0 + 2, at_dst(xr, 0), at_dst(xr, 0), mate)
    start(M0 + 3, at_dst(yr, 1), at_dst(yr, 1), mate)
    arrive(M0, at_dst(mr, 0))
    arrive(M0 + 1, at_dst(mr, 1))
    fill_dst(mr)

    arrive(X1, at_dst(xr, 1))
    start(M0 + 4, at_dst(xr, 1), at_dst(xr, 1), mate)
    arrive(Y0, at_dst(yr, 0))
    start(M0 + 5, at_dst(yr, 0), at_dst(yr, 0), mate)
    for way in (1, -1):
        line_wait(way, 0, 1)
        line_send(way, 1, 1)
    fill_dst(xr)
    fill_dst(yr)
    fill_src(c - 1)
    fill_src(c + 1)
    arrive(M0 + 2, at_dst(mx, 0))
    arrive(M0 + 4, at_dst(mx, 1))
    fill_dst(mx)
    arrive(M0 + 3, at_dst(my, 1))
    arrive(M0 + 5, at_dst(my, 0))
    fill_dst(my)

    arrive(YD, at_dst(dr, 0))
    start(M0 + 6, at_dst(dr, 0), at_dst(dr, 0), mate)
    arrive(XD, at_dst(dr, 1))
    start(M0 + 7, at_dst(dr, 1), at_dst(dr, 1), mate)
    for way in (1, -1):
        line_wait(way, 1, 0)
        line_send(way, 2, 0)
    fill_dst(dr)
    arrive(M0 + 6, at_dst(md, 0))
    arrive(M0 + 7, at_dst(md, 1))
    fill_dst(md)
    pick_all(o_tab, 1, go)

    for way in (1, -1):
        line_wait(way, 1, 1)
        line_send(way, 2, 1)
    fill_src(c - 2)
    fill_src(c + 2)
    eye = lax.broadcasted_iota(jnp.int32, (LANE, LANE), 0) == lax.broadcasted_iota(jnp.int32, (LANE, LANE), 1)
    cuts = ((0, LANE), (LANE, dim))

    def main_stage(low_row, size):
        def one_group(g, carry):
            pick(s_tab, 0, g, low_row, size)
            first = groups * low_row + g * size

            def query(i, inner):
                row = pl.multiple_of(i * QROWS, QROWS)
                rows = pl.ds(pl.multiple_of(first + row, QROWS), QROWS)
                score = None
                for half, (low, high) in enumerate(cuts):
                    near = lambda p: gs[pl.ds(row * 4 + p * 2 + half, QROWS, stride=4), :]
                    dense = lambda ref, p: ref[rows, p * WIDE + half * LANE : p * WIDE + (half + 1) * LANE].astype(F32)
                    sr, si, wr, wi = near(0), near(1), dense(gw, 0), dense(gw, 1)
                    qr = sr * wr - si * wi
                    qi = sr * wi + si * wr
                    add = qr * dense(go, 0) + qi * dense(go, 1)
                    score = add if score is None else score + add
                    qb[0, pl.ds(row, QROWS), low:high] = qr[:, : high - low].astype(BF16)
                    qb[1, pl.ds(row, QROWS), low:high] = qi[:, : high - low].astype(BF16)
                dots[pl.ds(row, QROWS), :] = score
                return inner

            lax.fori_loop(0, size // QROWS, query, 0)
            b = neg_i[g]
            near = lambda p: dstb[b, p]
            score = jnp.dot(qb[0, :size], near(0), preferred_element_type=F32)
            score = score + jnp.dot(qb[1, :size], near(1), preferred_element_type=F32)
            small = jnp.exp(-jnp.abs(score))
            soft = jnp.maximum(score, 0.0) + log1p_small(small)
            ratio = 1.0 / (1.0 + small)
            weight = jnp.where(score >= 0.0, ratio, small * ratio).astype(BF16)
            p = jnp.sum(dots[:size], 1, keepdims=True)
            p_small = jnp.exp(-jnp.abs(p))
            value = jnp.maximum(-p, 0.0) + log1p_small(p_small) + jnp.sum(soft, 1, keepdims=True) * (1.0 / NEGB)
            pull = jnp.where(p >= 0.0, p_small, 1.0) / (1.0 + p_small)
            for i in range(size // LANE):
                piece = value[i * LANE : (i + 1) * LANE]
                lossp[pl.ds((low_row // LANE + i) * groups + g, 1), :] = jnp.sum(jnp.where(eye, piece, 0.0), 0, keepdims=True)
            g_re = lax.dot_general(weight, near(0), nt, preferred_element_type=F32) * (1.0 / NEGB)
            g_im = lax.dot_general(weight, near(1), nt, preferred_element_type=F32) * (1.0 / NEGB)
            rows = pl.ds(pl.multiple_of(first, size), size)
            for half, (low, high) in enumerate(cuts):
                wide = high - low
                part = lambda q: gs[pl.ds(q * 2 + half, size, stride=4), :][:, :wide]
                lanes = lambda q: slice(q * WIDE + low, q * WIDE + high)
                d_re = g_re[:, low:high] - pull * go[rows, lanes(0)].astype(F32)
                d_im = g_im[:, low:high] - pull * go[rows, lanes(1)].astype(F32)
                s_re, s_im = part(0), part(1)
                gw[rows, lanes(0)] = (d_re * s_re + d_im * s_im).astype(BF16)
                gw[rows, lanes(1)] = (d_im * s_re - d_re * s_im).astype(BF16)
            return carry

        lax.fori_loop(0, groups, one_group, 0)

    tile = 8 * span

    def far_half(p):
        for way in (1, -1):
            line_wait(way, n_col - 2, p)
            shard = c - way * (n_col - 1)

            @pl.when(inside(shard))
            def _():
                fill_half(srcb, shard * per + p, (s_tab, shard * per + p))

    def terms(plane, low, high):
        ids = lax.broadcasted_iota(jnp.int32, (tile, high - low), 0) + plane * tile
        hot = jnp.where(ids == key[:, low:high], 1.0, 0.0).astype(BF16)
        return jnp.dot(hot, gw[low:high], preferred_element_type=F32)

    if len(stages) > 1:
        main_stage(*stages[0])
        far_half(0)
        main_stage(*stages[1])
        done = groups * stages[2][0]

        def begin(plane, carry):
            acc[plane] = (terms(plane, 0, done) + flag[...]).reshape(acc.shape[1:])
            return carry

        lax.fori_loop(0, n_col, begin, 0)
        far_half(1)
        main_stage(*stages[2])
    else:
        done = 0
        far_half(0)
        far_half(1)
        main_stage(*stages[0])

    home = [2, 1, 3, 0]
    S0 = M0 + 8
    spots = [(xp, (y * 2 + 1 - x)), (yp, ((1 - y) * 2 + x)), (dp, ((1 - y) * 2 + 1 - x))]
    order = [2, 0, 1]

    def pair_up(t):
        arrive(S0 + t, pairb.at[t])
        tot[t] = acc[(c + home[t]) % n_col, core] + pairb[t]
        for k in order:
            peer, there = spots[k]
            start(S0 + 4 + t * 3 + k, tot.at[t, there], inb.at[t, k], peer)

    def plane_sum(t):
        total = tot[t, chip]
        for k in range(3):
            arrive(S0 + 4 + t * 3 + k, inb.at[t, k])
            total = total + inb[t, k]
        return total

    for t in range(n_col):
        plane = (c + home[t]) % n_col
        part = terms(plane, done, edges).reshape(acc.shape[1:])
        acc[plane] = acc[plane] + part if done else part
        start(S0 + t, acc.at[plane, 1 - core], pairb.at[t], mate)
        if t:
            pair_up(t - 1)
    pair_up(n_col - 1)
    Z0 = S0 + 4 + n_col * 3
    for t in range(n_col - 1):
        zs[t] = plane_sum(t)
        start(Z0 + t, zs.at[t], zin.at[t], (r, (c + home[t]) % n_col))
    full = jnp.concatenate([lossp[i * groups : (i + 1) * groups] for i in range(group // LANE)], 1)
    high = full.astype(BF16).astype(F32)
    mid = (full - high).astype(BF16).astype(F32)
    low = full - high - mid
    shares = jnp.concatenate([high, mid, low, jnp.zeros_like(low)], 0).astype(BF16)
    which = lax.broadcasted_iota(jnp.int32, (groups, group), 0)

    def restore(g, carry):
        got = jnp.dot(shares, turn(g), preferred_element_type=F32)
        whole = got[:groups] + got[groups : 2 * groups] + got[2 * groups : 3 * groups]
        return jnp.where(which == g, whole, carry)

    back = lax.fori_loop(0, groups, restore, jnp.zeros((groups, group), F32))
    for g in range(groups):
        for i in range(group // LANE):
            at = g * (group // LANE) + i
            loss[at : at + 1, :] = back[g : g + 1, i * LANE : (i + 1) * LANE]
    total = plane_sum(n_col - 1)
    for t in range(n_col - 1):
        arrive(Z0 + t, zin.at[t])
        total = total + zin[t]
    grad[0] = total[:, :dim]
    grad[1] = total[:, WIDE : WIDE + dim]
    late[...] = total[:8, WIDE - LANE : WIDE]

    for cond, move in started:
        if cond is None:
            move.wait_send()
        else:
            pl.when(cond)(move.wait_send)


def step_call(n_row, n_col, fast, ent, rel, src_index, dst_index, rel_index, neg_block):
    edges, groups = src_index.shape[0], neg_block.shape[0]
    group = edges // groups
    parts, dim, count = ent.shape
    n_rel = rel.shape[2]
    span = n_rel // (n_row * n_col)
    chips = n_row // 2
    stages = ((0, 256), (256, 128), (384, 128)) if fast else ((0, group),)
    flat = lambda a: a.reshape(1, edges)
    smem = pl.BlockSpec(memory_space=pltpu.SMEM)
    vmem = pl.BlockSpec(memory_space=pltpu.VMEM)
    hbm = pl.BlockSpec(memory_space=pltpu.HBM)
    dma = pltpu.SemaphoreType.DMA
    copies = 4 * (n_col - 1) + 14 + 4 + n_col * 3 + n_col - 1
    return pl.pallas_call(
        functools.partial(step_kernel, n_col, group, stages),
        name="step" if fast else "step_late",
        out_shape=(
            jax.ShapeDtypeStruct((edges // LANE, LANE), F32),
            jax.ShapeDtypeStruct((parts, span, dim), F32),
            jax.ShapeDtypeStruct((8, LANE), F32),
        ),
        in_specs=[smem, vmem, vmem, vmem, hbm, hbm],
        out_specs=(vmem, vmem, vmem),
        scratch_shapes=[
            pltpu.VMEM((n_col * count // NEGB, parts, dim, NEGB), BF16),
            pltpu.VMEM((n_row * count // NEGB, parts, dim, NEGB), BF16),
            pltpu.VMEM(rel.shape, BF16),
            pltpu.VMEM((n_col * count, 4, LANE), F32),
            pltpu.VMEM((n_row * count, 4, LANE), F32),
            pltpu.VMEM((n_rel, 4, LANE), F32),
            pltpu.VMEM((group * 4, LANE), F32),
            pltpu.VMEM((edges, 2 * WIDE), BF16),
            pltpu.VMEM((edges, 2 * WIDE), BF16),
            pltpu.VMEM((parts, group, dim), BF16),
            pltpu.VMEM((group, LANE), F32),
            pltpu.VMEM((1, edges), jnp.int32),
            pltpu.VMEM((groups, group), jnp.int32),
            pltpu.VMEM((6 * groups, group), F32),
            pltpu.VMEM((3, groups, group), jnp.int32),
            pltpu.VMEM((3 * edges // LANE, LANE), jnp.int32),
            pltpu.SMEM((3 * edges // LANE, LANE), jnp.int32),
            pltpu.VMEM((edges // LANE, LANE), F32),
            pltpu.VMEM((1, 2 * WIDE), F32),
            pltpu.VMEM((n_col, 2, chips, span, 2 * WIDE), F32),
            pltpu.VMEM((n_col, chips, span, 2 * WIDE), F32),
            pltpu.VMEM((n_col, chips, span, 2 * WIDE), F32),
            pltpu.VMEM((n_col, 3, span, 2 * WIDE), F32),
            pltpu.VMEM((n_col - 1, span, 2 * WIDE), F32),
            pltpu.VMEM((n_col - 1, span, 2 * WIDE), F32),
            dma((4,)), dma((copies,)), dma((copies,)),
        ],
        compiler_params=pltpu.CompilerParams(
            collective_id=0 if fast else 1, has_side_effects=True, vmem_limit_bytes=67043328
        ),
    )(neg_block, flat(src_index), flat(dst_index), flat(rel_index), ent, rel)


def body(n_row, n_col, entities, relations, src_index, dst_index, rel_index, neg_block):
    dim = entities.shape[2]
    count = entities.shape[1]
    args = (entities, relations, src_index, dst_index, rel_index, neg_block)
    fits = LANE < dim < WIDE and (n_row + n_col) * count * 4 * LANE * 4 <= 26 * 2**20
    if n_row != 8 or n_col != 4 or count != 2 * NEGB or not fits:
        return wide_body(*args)
    if src_index.shape[0] != 8 * neg_block.shape[0] * 64 or neg_block.shape[0] != 8:
        return wide_body(*args)
    flip = lambda a: jnp.transpose(a, (0, 2, 1))
    whole = (flip(entities), flip(relations), src_index, dst_index, rel_index, neg_block)
    edge_loss, grad, late = step_call(n_row, n_col, True, *whole)
    edge_loss, grad = lax.cond(
        late[0, LANE - 1] > 0.0,
        lambda: tuple(step_call(n_row, n_col, False, *whole)[:2]),
        lambda: (edge_loss, grad),
    )
    edge_loss, grad = settle(edge_loss, grad)
    return edge_loss.reshape(-1), grad


def settle_kernel(loss_in, grad_in, loss, grad):
    loss[...] = loss_in[...]
    grad[...] = grad_in[...]


def settle(edge_loss, grad):
    shape = lambda a: jax.ShapeDtypeStruct(a.shape, a.dtype)
    vmem = pl.BlockSpec(memory_space=pltpu.VMEM)
    return pl.pallas_call(
        settle_kernel, name="settle", out_shape=(shape(edge_loss), shape(grad)),
        in_specs=[vmem, vmem], out_specs=(vmem, vmem),
    )(edge_loss, grad)


def bucket_terms(picked_src, picked_dst, negatives, relations, rel_ids):
    onehot = (rel_ids[:, None] == jnp.arange(relations.shape[1], dtype=jnp.int32)[None, :]).astype(
        jnp.bfloat16
    )
    rel_re = jnp.dot(onehot, relations[0], preferred_element_type=jnp.float32)
    rel_im = jnp.dot(onehot, relations[1], preferred_element_type=jnp.float32)
    src_re = picked_src[0].astype(jnp.float32)
    src_im = picked_src[1].astype(jnp.float32)
    dst_re = picked_dst[0].astype(jnp.float32)
    dst_im = picked_dst[1].astype(jnp.float32)
    query_re = src_re * rel_re - src_im * rel_im
    query_im = src_re * rel_im + src_im * rel_re
    pos_score = jnp.sum(query_re * dst_re, 1) + jnp.sum(query_im * dst_im, 1)
    groups = negatives.shape[1]
    dim = query_re.shape[1]
    qre_b = query_re.astype(jnp.bfloat16).reshape(groups, -1, dim)
    qim_b = query_im.astype(jnp.bfloat16).reshape(groups, -1, dim)
    neg_score = jnp.einsum(
        "kcd,knd->kcn", qre_b, negatives[0], preferred_element_type=jnp.float32
    ) + jnp.einsum("kcd,knd->kcn", qim_b, negatives[1], preferred_element_type=jnp.float32)
    edge_loss = jax.nn.softplus(-pos_score) + jnp.mean(jax.nn.softplus(neg_score), -1).reshape(-1)
    weights = (jax.nn.sigmoid(neg_score) / NEGB).astype(jnp.bfloat16)
    gneg_re = jnp.einsum(
        "kcn,knd->kcd", weights, negatives[0], preferred_element_type=jnp.float32
    ).reshape(-1, dim)
    gneg_im = jnp.einsum(
        "kcn,knd->kcd", weights, negatives[1], preferred_element_type=jnp.float32
    ).reshape(-1, dim)
    pull = jax.nn.sigmoid(-pos_score)[:, None]
    grad_re = gneg_re - pull * dst_re
    grad_im = gneg_im - pull * dst_im
    term_re = (grad_re * src_re + grad_im * src_im).astype(jnp.bfloat16)
    term_im = (grad_im * src_re - grad_re * src_im).astype(jnp.bfloat16)
    dims = (((0,), (0,)), ((), ()))
    rel_grad = jnp.stack(
        [
            lax.dot_general(onehot, term_re, dims, preferred_element_type=jnp.float32),
            lax.dot_general(onehot, term_im, dims, preferred_element_type=jnp.float32),
        ],
        0,
    )
    return (edge_loss, rel_grad)


def wide_body(entities, relations, src_index, dst_index, rel_index, neg_block):
    dim = entities.shape[2]
    source_rows = lax.all_gather(entities, "col", axis=1, tiled=True)
    picked_src = jnp.take(source_rows, src_index, axis=1)
    target_rows = lax.all_gather(entities, "row", axis=1, tiled=True)
    picked_dst = jnp.take(target_rows, dst_index, axis=1)
    negatives = jnp.take(target_rows.reshape(2, -1, NEGB, dim), neg_block, axis=1)
    edge_loss, rel_grad = bucket_terms(picked_src, picked_dst, negatives, relations, rel_index)
    row_share = lax.psum_scatter(rel_grad, "row", scatter_dimension=1, tiled=True)
    grad_share = lax.psum_scatter(row_share, "col", scatter_dimension=1, tiled=True)
    return (edge_loss, grad_share)


def solution(mesh):
    placed = (
        P(None, ("row", "col"), None),
        P(),
        P(("row", "col")),
        P(("row", "col")),
        P(("row", "col")),
        P(("row", "col")),
    )
    return jax.shard_map(
        functools.partial(body, mesh.shape["row"], mesh.shape["col"]),
        mesh=mesh,
        in_specs=placed,
        out_specs=(P(("row", "col")), P(None, ("row", "col"), None)),
        check_vma=False,
    )
```

```python
import functools

import jax
import jax.numpy as jnp
from jax import lax
from jax.experimental import pallas as pl
from jax.experimental.pallas import tpu as pltpu
from jax.sharding import PartitionSpec as P

NEGB = 512
LANE = 128
WIDE = 256
MESH = pl.DeviceIdType.MESH
F32 = jnp.float32
BF16 = jnp.bfloat16
PICKS = 32
QROWS = 128
PROWS = 128


def log1p_small(u):
    return jnp.where(u < 2.0**-9, u - 0.5 * u * u, jnp.log(1.0 + u))


def step_kernel(
    n_col, group, stages, neg_i, src_row, dst_row, rel_row, ent, rel, loss, grad, late,
    srcb, dstb, relb, s_tab, o_tab, w_tab, gs, go, gw, qb, dots, key, spot, moved, order_v, order_t, order_s, lossp, flag,
    acc, pairb, tot, inb, zs, zin, loc_sem, send_sem, recv_sem,
):
    r, c = lax.axis_index("row"), lax.axis_index("col")
    chip, core = r // 2, r % 2
    y, x = chip // 2, chip % 2
    row_of = lambda yy, xx, k: (yy * 2 + xx) * 2 + k
    xr, yr, dr = row_of(y, 1 - x, core), row_of(1 - y, x, core), row_of(1 - y, 1 - x, core)
    mr, mx, my, md = (row_of(yy, xx, 1 - core) for yy, xx in ((y, x), (y, 1 - x), (1 - y, x), (1 - y, 1 - x)))
    mate, xp, yp, dp = (mr, c), (xr, c), (yr, c), (dr, c)
    dim, count = ent.shape[1], ent.shape[2]
    n_rel = rel.shape[2]
    groups = neg_i.shape[0]
    edges = gw.shape[0]
    per = count // NEGB
    rest = dim - LANE

    barrier = pltpu.get_barrier_semaphore()
    peers = [mate, xp, yp, dp] + [(r, (c + b) % n_col) for b in range(1, n_col)]
    for peer in peers:
        pl.semaphore_signal(barrier, inc=1, device_id=peer, device_id_type=MESH)
    pl.semaphore_wait(barrier, len(peers))

    started = []

    def copy(k, src, dst, peer):
        return pltpu.make_async_remote_copy(
            src_ref=src, dst_ref=dst, send_sem=send_sem.at[k], recv_sem=recv_sem.at[k],
            device_id=peer, device_id_type=MESH,
        )

    def start(k, src, dst, peer):
        move = copy(k, src, dst, peer)
        move.start()
        started.append((None, move))

    def arrive(k, dst):
        copy(k, dst, dst, mate).wait_recv()

    own = lambda p: ent.at[:, :, p * NEGB : (p + 1) * NEGB]
    inside = lambda v: jnp.logical_and(v >= 0, v < n_col)

    def line_id(way, age, part):
        return ((0 if way > 0 else n_col - 1) + age) * 2 + part

    def line_send(way, age, part):
        shard = c - way * age
        cond = jnp.logical_and(inside(c + way), inside(shard))
        src = own(part) if age == 0 else srcb.at[shard * per + part]
        move = copy(line_id(way, age, part), src, srcb.at[shard * per + part], (r, c + way))

        @pl.when(cond)
        def _():
            move.start()

        started.append((cond, move))

    def line_wait(way, age, part):
        shard = c - way * (age + 1)

        @pl.when(inside(shard))
        def _():
            arrive(line_id(way, age, part), srcb.at[shard * per + part])

    base = 4 * (n_col - 1)
    X0, X1, Y0, Y1, XD, YD, M0 = (base + k for k in range(7))
    at_dst = lambda i, p: dstb.at[i * per + p]

    line_send(1, 0, 0)
    line_send(-1, 0, 0)
    start(X0, own(0), at_dst(r, 0), xp)
    start(Y1, own(1), at_dst(r, 1), yp)
    local_rel = pltpu.make_async_copy(rel, relb, loc_sem.at[0])
    local_ent = [pltpu.make_async_copy(own(p), at_dst(r, p), loc_sem.at[1 + p]) for p in range(per)]
    local_rel.start()
    for move in local_ent:
        move.start()
    line_send(1, 0, 1)
    line_send(-1, 0, 1)
    start(X1, own(1), at_dst(r, 1), xp)
    start(Y0, own(0), at_dst(r, 0), yp)
    start(M0, own(0), at_dst(r, 0), mate)
    start(M0 + 1, own(1), at_dst(r, 1), mate)

    def fill(read, targets):
        def step(j, carry):
            for both in range(4):
                col = pl.multiple_of(j * (4 * LANE) + both * LANE, LANE)
                for part in range(2):
                    low = read(part, slice(0, LANE), col).astype(F32).T
                    high = read(part, slice(LANE, dim), col).astype(F32)
                    high = jnp.concatenate([high, jnp.zeros((LANE - rest, LANE), F32)], 0).T
                    for table, first, _ in targets:
                        flat = table.reshape(table.shape[0] * 4, LANE)
                        at = first + col * 4 + part * 2
                        flat[pl.ds(at, LANE, stride=4), :] = low
                        flat[pl.ds(at + 1, LANE, stride=4), :] = high
            return carry

        lax.fori_loop(0, targets[0][2] // (4 * LANE), step, 0)

    def fill_half(buf, half, *tables):
        fill(
            lambda p, rows, col: buf[half, p, rows, pl.ds(col, LANE)],
            [(table, shard * (NEGB * 4), NEGB) for table, shard in tables],
        )

    def fill_dst(shard):
        for p in range(per):
            half = shard * per + p
            fill_half(dstb, half, (o_tab, half))

    def fill_src(shard):
        @pl.when(inside(shard))
        def _():
            for p in range(per):
                half = shard * per + p
                fill_half(srcb, half, (s_tab, half))

    def pick(table, kind, g, low, rows):
        top = table.shape[0] - 1
        keep = (lambda v: v & top) if top & (top + 1) == 0 else (lambda v: jnp.clip(v, 0, top))
        start_row = kind * (edges // LANE) + low // LANE * groups + g

        def step(i, carry):
            row = start_row + i * groups
            for part in range(0, LANE, PICKS):
                got = [table[keep(order_s[row, part + u])] for u in range(PICKS)]
                for u in range(PICKS):
                    gs[pl.ds(pl.multiple_of((i * LANE + part + u) * 4, 4), 4), :] = got[u]
            return carry

        lax.fori_loop(0, rows // LANE, step, 0)

    def pick_all(table, kind, out):
        for low, rows in stages:
            def one(g, carry, low=low, rows=rows):
                pick(table, kind, g, low, rows)

                def pack(i, inner):
                    row = pl.multiple_of(i * PROWS, PROWS)
                    at = pl.ds(pl.multiple_of(groups * low + g * rows + row, PROWS), PROWS)
                    for k in range(4):
                        out[at, k * LANE : (k + 1) * LANE] = gs[pl.ds(row * 4 + k, PROWS, stride=4), :].astype(BF16)
                    return inner

                lax.fori_loop(0, rows // PROWS, pack, 0)
                return carry

            lax.fori_loop(0, groups, one, 0)

    span = n_rel // (8 * n_col)
    for g in range(groups):
        cut = slice(g * group, (g + 1) * group)
        for kind, ref in enumerate((src_row, dst_row, rel_row)):
            order_v[kind, g : g + 1, :] = ref[:, cut]
    halves = lax.div(order_v[0], NEGB)
    far = jnp.abs(lax.div(halves, per) - c) == n_col - 1
    last = jnp.logical_and(far, lax.rem(halves, per) == per - 1)
    early = jnp.where(far, 0.0, 1.0)
    middle = jnp.where(last, 0.0, 1.0) - early
    lane_id = lax.broadcasted_iota(jnp.int32, (groups, group), 1).astype(F32)
    before = lax.broadcasted_iota(jnp.int32, (group, group), 0) < lax.broadcasted_iota(jnp.int32, (group, group), 1)
    ahead = jnp.dot(
        jnp.concatenate([early, middle], 0).astype(BF16), jnp.where(before, 1.0, 0.0).astype(BF16),
        preferred_element_type=F32,
    )
    ahead0, ahead1 = ahead[:groups], ahead[groups:]
    n_early = jnp.sum(early, 1, keepdims=True)
    n_middle = jnp.sum(middle, 1, keepdims=True)
    place = jnp.where(
        far, jnp.where(last, n_early + n_middle + lane_id - ahead0 - ahead1, n_early + ahead1), ahead0
    )
    spot[...] = place.astype(jnp.int32)
    if len(stages) > 1:
        short = jnp.maximum(
            jnp.where(n_early < float(stages[1][0]), 1.0, 0.0),
            jnp.where(n_early + n_middle < float(stages[2][0]), 1.0, 0.0),
        )
        lanes = lax.broadcasted_iota(jnp.int32, (1, 2 * WIDE), 1)
        flag[...] = jnp.where(lanes == WIDE - 1, jnp.sum(short, 0, keepdims=True), 0.0)
    else:
        flag[...] = jnp.zeros_like(flag)

    def turn(g):
        ids = lax.broadcasted_iota(jnp.int32, (group, group), 0)
        return jnp.where(ids == spot[pl.ds(g, 1), :], 1.0, 0.0).astype(BF16)

    split = []
    for kind in range(3):
        split += [lax.div(order_v[kind], LANE), lax.rem(order_v[kind], LANE)]
    moved[...] = jnp.concatenate(split, 0).astype(F32)
    pieces = moved[...].astype(BF16)
    mine = lax.rem(lax.broadcasted_iota(jnp.int32, (6 * groups, group), 0), groups)
    nt = (((1,), (1,)), ((), ()))

    def reorder(g, carry):
        got = lax.dot_general(pieces, turn(g), nt, preferred_element_type=F32)
        moved[...] = jnp.where(mine == g, got, moved[...])
        return carry

    lax.fori_loop(0, groups, reorder, 0)
    for kind in range(3):
        at = kind * 2 * groups
        order_v[kind] = (moved[at : at + groups] * LANE + moved[at + groups : at + 2 * groups]).astype(jnp.int32)
    blocks = group // LANE
    for kind in range(3):
        for i in range(blocks):
            at = (kind * blocks + i) * groups
            order_t[at : at + groups, :] = order_v[kind, :, i * LANE : (i + 1) * LANE]
    to_scalar = pltpu.make_async_copy(order_t, order_s, loc_sem.at[3])
    to_scalar.start()
    rel_ids = order_v[2]
    row_part = lax.div(rel_ids, n_col * span)
    keys = (
        lax.rem(lax.div(rel_ids, span), n_col) * (8 * span)
        + lax.rem(row_part, 2) * (4 * span) + lax.div(row_part, 2) * span + lax.rem(rel_ids, span)
    )
    for low, rows in stages:
        for g in range(groups):
            at = groups * low + g * rows
            key[:, at : at + rows] = keys[g : g + 1, low : low + rows]
    to_scalar.wait()

    local_rel.wait()
    fill(lambda p, rows, col: relb[p, rows, pl.ds(col, LANE)], [(w_tab, 0, n_rel)])
    pick_all(w_tab, 2, gw)
    for move in local_ent:
        move.wait()
    for p in range(per):
        fill_half(dstb, r * per + p, (o_tab, r * per + p), (s_tab, c * per + p))

    arrive(X0, at_dst(xr, 0))
    start(YD, at_dst(xr, 0), at_dst(xr, 0), yp)
    arrive(Y1, at_dst(yr, 1))
    start(XD, at_dst(yr, 1), at_dst(yr, 1), xp)
    for way in (1, -1):
        line_wait(way, 0, 0)
        line_send(way, 1, 0)
    start(M0 + 2, at_dst(xr, 0), at_dst(xr, 0), mate)
    start(M0 + 3, at_dst(yr, 1), at_dst(yr, 1), mate)
    arrive(M0, at_dst(mr, 0))
    arrive(M0 + 1, at_dst(mr, 1))
    fill_dst(mr)

    arrive(X1, at_dst(xr, 1))
    start(M0 + 4, at_dst(xr, 1), at_dst(xr, 1), mate)
    arrive(Y0, at_dst(yr, 0))
    start(M0 + 5, at_dst(yr, 0), at_dst(yr, 0), mate)
    for way in (1, -1):
        line_wait(way, 0, 1)
        line_send(way, 1, 1)
    fill_dst(xr)
    fill_dst(yr)
    fill_src(c - 1)
    fill_src(c + 1)
    arrive(M0 + 2, at_dst(mx, 0))
    arrive(M0 + 4, at_dst(mx, 1))
    fill_dst(mx)
    arrive(M0 + 3, at_dst(my, 1))
    arrive(M0 + 5, at_dst(my, 0))
    fill_dst(my)

    arrive(YD, at_dst(dr, 0))
    start(M0 + 6, at_dst(dr, 0), at_dst(dr, 0), mate)
    arrive(XD, at_dst(dr, 1))
    start(M0 + 7, at_dst(dr, 1), at_dst(dr, 1), mate)
    for way in (1, -1):
        line_wait(way, 1, 0)
        line_send(way, 2, 0)
    fill_dst(dr)
    arrive(M0 + 6, at_dst(md, 0))
    arrive(M0 + 7, at_dst(md, 1))
    fill_dst(md)
    pick_all(o_tab, 1, go)

    for way in (1, -1):
        line_wait(way, 1, 1)
        line_send(way, 2, 1)
    fill_src(c - 2)
    fill_src(c + 2)
    eye = lax.broadcasted_iota(jnp.int32, (LANE, LANE), 0) == lax.broadcasted_iota(jnp.int32, (LANE, LANE), 1)
    cuts = ((0, LANE), (LANE, dim))

    def main_stage(low_row, size):
        def one_group(g, carry):
            pick(s_tab, 0, g, low_row, size)
            first = groups * low_row + g * size

            def query(i, inner):
                row = pl.multiple_of(i * QROWS, QROWS)
                rows = pl.ds(pl.multiple_of(first + row, QROWS), QROWS)
                score = None
                for half, (low, high) in enumerate(cuts):
                    near = lambda p: gs[pl.ds(row * 4 + p * 2 + half, QROWS, stride=4), :]
                    dense = lambda ref, p: ref[rows, p * WIDE + half * LANE : p * WIDE + (half + 1) * LANE].astype(F32)
                    sr, si, wr, wi = near(0), near(1), dense(gw, 0), dense(gw, 1)
                    qr = sr * wr - si * wi
                    qi = sr * wi + si * wr
                    add = qr * dense(go, 0) + qi * dense(go, 1)
                    score = add if score is None else score + add
                    qb[0, pl.ds(row, QROWS), low:high] = qr[:, : high - low].astype(BF16)
                    qb[1, pl.ds(row, QROWS), low:high] = qi[:, : high - low].astype(BF16)
                dots[pl.ds(row, QROWS), :] = score
                return inner

            lax.fori_loop(0, size // QROWS, query, 0)
            b = neg_i[g]
            near = lambda p: dstb[b, p]
            score = jnp.dot(qb[0, :size], near(0), preferred_element_type=F32)
            score = score + jnp.dot(qb[1, :size], near(1), preferred_element_type=F32)
            small = jnp.exp(-jnp.abs(score))
            soft = jnp.maximum(score, 0.0) + log1p_small(small)
            ratio = 1.0 / (1.0 + small)
            weight = jnp.where(score >= 0.0, ratio, small * ratio).astype(BF16)
            p = jnp.sum(dots[:size], 1, keepdims=True)
            p_small = jnp.exp(-jnp.abs(p))
            value = jnp.maximum(-p, 0.0) + log1p_small(p_small) + jnp.sum(soft, 1, keepdims=True) * (1.0 / NEGB)
            pull = jnp.where(p >= 0.0, p_small, 1.0) / (1.0 + p_small)
            for i in range(size // LANE):
                piece = value[i * LANE : (i + 1) * LANE]
                lossp[pl.ds((low_row // LANE + i) * groups + g, 1), :] = jnp.sum(jnp.where(eye, piece, 0.0), 0, keepdims=True)
            g_re = lax.dot_general(weight, near(0), nt, preferred_element_type=F32) * (1.0 / NEGB)
            g_im = lax.dot_general(weight, near(1), nt, preferred_element_type=F32) * (1.0 / NEGB)
            rows = pl.ds(pl.multiple_of(first, size), size)
            for half, (low, high) in enumerate(cuts):
                wide = high - low
                part = lambda q: gs[pl.ds(q * 2 + half, size, stride=4), :][:, :wide]
                lanes = lambda q: slice(q * WIDE + low, q * WIDE + high)
                d_re = g_re[:, low:high] - pull * go[rows, lanes(0)].astype(F32)
                d_im = g_im[:, low:high] - pull * go[rows, lanes(1)].astype(F32)
                s_re, s_im = part(0), part(1)
                gw[rows, lanes(0)] = (d_re * s_re + d_im * s_im).astype(BF16)
                gw[rows, lanes(1)] = (d_im * s_re - d_re * s_im).astype(BF16)
            return carry

        lax.fori_loop(0, groups, one_group, 0)

    tile = 8 * span

    def far_half(p):
        for way in (1, -1):
            line_wait(way, n_col - 2, p)
            shard = c - way * (n_col - 1)

            @pl.when(inside(shard))
            def _():
                fill_half(srcb, shard * per + p, (s_tab, shard * per + p))

    def terms(plane, low, high):
        ids = lax.broadcasted_iota(jnp.int32, (tile, high - low), 0) + plane * tile
        hot = jnp.where(ids == key[:, low:high], 1.0, 0.0).astype(BF16)
        return jnp.dot(hot, gw[low:high], preferred_element_type=F32)

    if len(stages) > 1:
        main_stage(*stages[0])
        far_half(0)
        main_stage(*stages[1])
        done = groups * stages[2][0]

        def begin(plane, carry):
            acc[plane] = (terms(plane, 0, done) + flag[...]).reshape(acc.shape[1:])
            return carry

        lax.fori_loop(0, n_col, begin, 0)
        far_half(1)
        main_stage(*stages[2])
    else:
        done = 0
        far_half(0)
        far_half(1)
        main_stage(*stages[0])

    home = [2, 1, 3, 0]
    S0 = M0 + 8
    spots = [(xp, (y * 2 + 1 - x)), (yp, ((1 - y) * 2 + x)), (dp, ((1 - y) * 2 + 1 - x))]
    order = [2, 0, 1]

    def pair_up(t):
        arrive(S0 + t, pairb.at[t])
        tot[t] = acc[(c + home[t]) % n_col, core] + pairb[t]
        for k in order:
            peer, there = spots[k]
            start(S0 + 4 + t * 3 + k, tot.at[t, there], inb.at[t, k], peer)

    def plane_sum(t):
        total = tot[t, chip]
        for k in range(3):
            arrive(S0 + 4 + t * 3 + k, inb.at[t, k])
            total = total + inb[t, k]
        return total

    for t in range(n_col):
        plane = (c + home[t]) % n_col
        part = terms(plane, done, edges).reshape(acc.shape[1:])
        acc[plane] = acc[plane] + part if done else part
        start(S0 + t, acc.at[plane, 1 - core], pairb.at[t], mate)
        if t:
            pair_up(t - 1)
    pair_up(n_col - 1)
    Z0 = S0 + 4 + n_col * 3
    for t in range(n_col - 1):
        zs[t] = plane_sum(t)
        start(Z0 + t, zs.at[t], zin.at[t], (r, (c + home[t]) % n_col))
    full = jnp.concatenate([lossp[i * groups : (i + 1) * groups] for i in range(group // LANE)], 1)
    high = full.astype(BF16).astype(F32)
    mid = (full - high).astype(BF16).astype(F32)
    low = full - high - mid
    shares = jnp.concatenate([high, mid, low, jnp.zeros_like(low)], 0).astype(BF16)
    which = lax.broadcasted_iota(jnp.int32, (groups, group), 0)

    def restore(g, carry):
        got = jnp.dot(shares, turn(g), preferred_element_type=F32)
        whole = got[:groups] + got[groups : 2 * groups] + got[2 * groups : 3 * groups]
        return jnp.where(which == g, whole, carry)

    back = lax.fori_loop(0, groups, restore, jnp.zeros((groups, group), F32))
    for g in range(groups):
        for i in range(group // LANE):
            at = g * (group // LANE) + i
            loss[at : at + 1, :] = back[g : g + 1, i * LANE : (i + 1) * LANE]
    total = plane_sum(n_col - 1)
    for t in range(n_col - 1):
        arrive(Z0 + t, zin.at[t])
        total = total + zin[t]
    grad[0] = total[:, :dim]
    grad[1] = total[:, WIDE : WIDE + dim]
    late[...] = total[:8, WIDE - LANE : WIDE]

    for cond, move in started:
        if cond is None:
            move.wait_send()
        else:
            pl.when(cond)(move.wait_send)


def step_call(n_row, n_col, fast, ent, rel, src_index, dst_index, rel_index, neg_block):
    edges, groups = src_index.shape[0], neg_block.shape[0]
    group = edges // groups
    parts, dim, count = ent.shape
    n_rel = rel.shape[2]
    span = n_rel // (n_row * n_col)
    chips = n_row // 2
    stages = ((0, 256), (256, 128), (384, 128)) if fast else ((0, group),)
    flat = lambda a: a.reshape(1, edges)
    smem = pl.BlockSpec(memory_space=pltpu.SMEM)
    vmem = pl.BlockSpec(memory_space=pltpu.VMEM)
    hbm = pl.BlockSpec(memory_space=pltpu.HBM)
    dma = pltpu.SemaphoreType.DMA
    copies = 4 * (n_col - 1) + 14 + 4 + n_col * 3 + n_col - 1
    return pl.pallas_call(
        functools.partial(step_kernel, n_col, group, stages),
        name="step" if fast else "step_late",
        out_shape=(
            jax.ShapeDtypeStruct((edges // LANE, LANE), F32),
            jax.ShapeDtypeStruct((parts, span, dim), F32),
            jax.ShapeDtypeStruct((8, LANE), F32),
        ),
        in_specs=[smem, vmem, vmem, vmem, hbm, hbm],
        out_specs=(vmem, vmem, vmem),
        scratch_shapes=[
            pltpu.VMEM((n_col * count // NEGB, parts, dim, NEGB), BF16),
            pltpu.VMEM((n_row * count // NEGB, parts, dim, NEGB), BF16),
            pltpu.VMEM(rel.shape, BF16),
            pltpu.VMEM((n_col * count, 4, LANE), F32),
            pltpu.VMEM((n_row * count, 4, LANE), F32),
            pltpu.VMEM((n_rel, 4, LANE), F32),
            pltpu.VMEM((group * 4, LANE), F32),
            pltpu.VMEM((edges, 2 * WIDE), BF16),
            pltpu.VMEM((edges, 2 * WIDE), BF16),
            pltpu.VMEM((parts, group, dim), BF16),
            pltpu.VMEM((group, LANE), F32),
            pltpu.VMEM((1, edges), jnp.int32),
            pltpu.VMEM((groups, group), jnp.int32),
            pltpu.VMEM((6 * groups, group), F32),
            pltpu.VMEM((3, groups, group), jnp.int32),
            pltpu.VMEM((3 * edges // LANE, LANE), jnp.int32),
            pltpu.SMEM((3 * edges // LANE, LANE), jnp.int32),
            pltpu.VMEM((edges // LANE, LANE), F32),
            pltpu.VMEM((1, 2 * WIDE), F32),
            pltpu.VMEM((n_col, 2, chips, span, 2 * WIDE), F32),
            pltpu.VMEM((n_col, chips, span, 2 * WIDE), F32),
            pltpu.VMEM((n_col, chips, span, 2 * WIDE), F32),
            pltpu.VMEM((n_col, 3, span, 2 * WIDE), F32),
            pltpu.VMEM((n_col - 1, span, 2 * WIDE), F32),
            pltpu.VMEM((n_col - 1, span, 2 * WIDE), F32),
            dma((4,)), dma((copies,)), dma((copies,)),
        ],
        compiler_params=pltpu.CompilerParams(
            collective_id=0 if fast else 1, has_side_effects=True, vmem_limit_bytes=67043328
        ),
    )(neg_block, flat(src_index), flat(dst_index), flat(rel_index), ent, rel)


def body(n_row, n_col, entities, relations, src_index, dst_index, rel_index, neg_block):
    dim = entities.shape[2]
    count = entities.shape[1]
    args = (entities, relations, src_index, dst_index, rel_index, neg_block)
    fits = LANE < dim < WIDE and (n_row + n_col) * count * 4 * LANE * 4 <= 26 * 2**20
    if n_row != 8 or n_col != 4 or count != 2 * NEGB or not fits:
        return wide_body(*args)
    if src_index.shape[0] != 8 * neg_block.shape[0] * 64 or neg_block.shape[0] != 8:
        return wide_body(*args)
    flip = lambda a: jnp.transpose(a, (0, 2, 1))
    whole = (flip(entities), flip(relations), src_index, dst_index, rel_index, neg_block)
    edge_loss, grad, late = step_call(n_row, n_col, True, *whole)
    edge_loss, grad = lax.cond(
        late[0, LANE - 1] > 0.0,
        lambda: tuple(step_call(n_row, n_col, False, *whole)[:2]),
        lambda: (edge_loss, grad),
    )
    edge_loss, grad = settle(edge_loss, grad)
    return edge_loss.reshape(-1), grad


def settle_kernel(loss_in, grad_in, loss, grad):
    loss[...] = loss_in[...]
    grad[...] = grad_in[...]


def settle(edge_loss, grad):
    shape = lambda a: jax.ShapeDtypeStruct(a.shape, a.dtype)
    vmem = pl.BlockSpec(memory_space=pltpu.VMEM)
    return pl.pallas_call(
        settle_kernel, name="settle", out_shape=(shape(edge_loss), shape(grad)),
        in_specs=[vmem, vmem], out_specs=(vmem, vmem),
    )(edge_loss, grad)


def bucket_terms(picked_src, picked_dst, negatives, relations, rel_ids):
    onehot = (rel_ids[:, None] == jnp.arange(relations.shape[1], dtype=jnp.int32)[None, :]).astype(
        jnp.bfloat16
    )
    rel_re = jnp.dot(onehot, relations[0], preferred_element_type=jnp.float32)
    rel_im = jnp.dot(onehot, relations[1], preferred_element_type=jnp.float32)
    src_re = picked_src[0].astype(jnp.float32)
    src_im = picked_src[1].astype(jnp.float32)
    dst_re = picked_dst[0].astype(jnp.float32)
    dst_im = picked_dst[1].astype(jnp.float32)
    query_re = src_re * rel_re - src_im * rel_im
    query_im = src_re * rel_im + src_im * rel_re
    pos_score = jnp.sum(query_re * dst_re, 1) + jnp.sum(query_im * dst_im, 1)
    groups = negatives.shape[1]
    dim = query_re.shape[1]
    qre_b = query_re.astype(jnp.bfloat16).reshape(groups, -1, dim)
    qim_b = query_im.astype(jnp.bfloat16).reshape(groups, -1, dim)
    neg_score = jnp.einsum(
        "kcd,knd->kcn", qre_b, negatives[0], preferred_element_type=jnp.float32
    ) + jnp.einsum("kcd,knd->kcn", qim_b, negatives[1], preferred_element_type=jnp.float32)
    edge_loss = jax.nn.softplus(-pos_score) + jnp.mean(jax.nn.softplus(neg_score), -1).reshape(-1)
    weights = (jax.nn.sigmoid(neg_score) / NEGB).astype(jnp.bfloat16)
    gneg_re = jnp.einsum(
        "kcn,knd->kcd", weights, negatives[0], preferred_element_type=jnp.float32
    ).reshape(-1, dim)
    gneg_im = jnp.einsum(
        "kcn,knd->kcd", weights, negatives[1], preferred_element_type=jnp.float32
    ).reshape(-1, dim)
    pull = jax.nn.sigmoid(-pos_score)[:, None]
    grad_re = gneg_re - pull * dst_re
    grad_im = gneg_im - pull * dst_im
    term_re = (grad_re * src_re + grad_im * src_im).astype(jnp.bfloat16)
    term_im = (grad_im * src_re - grad_re * src_im).astype(jnp.bfloat16)
    dims = (((0,), (0,)), ((), ()))
    rel_grad = jnp.stack(
        [
            lax.dot_general(onehot, term_re, dims, preferred_element_type=jnp.float32),
            lax.dot_general(onehot, term_im, dims, preferred_element_type=jnp.float32),
        ],
        0,
    )
    return (edge_loss, rel_grad)


def wide_body(entities, relations, src_index, dst_index, rel_index, neg_block):
    dim = entities.shape[2]
    source_rows = lax.all_gather(entities, "col", axis=1, tiled=True)
    picked_src = jnp.take(source_rows, src_index, axis=1)
    target_rows = lax.all_gather(entities, "row", axis=1, tiled=True)
    picked_dst = jnp.take(target_rows, dst_index, axis=1)
    negatives = jnp.take(target_rows.reshape(2, -1, NEGB, dim), neg_block, axis=1)
    edge_loss, rel_grad = bucket_terms(picked_src, picked_dst, negatives, relations, rel_index)
    row_share = lax.psum_scatter(rel_grad, "row", scatter_dimension=1, tiled=True)
    grad_share = lax.psum_scatter(row_share, "col", scatter_dimension=1, tiled=True)
    return (edge_loss, grad_share)


def solution(mesh):
    placed = (
        P(None, ("row", "col"), None),
        P(),
        P(("row", "col")),
        P(("row", "col")),
        P(("row", "col")),
        P(("row", "col")),
    )
    return jax.shard_map(
        functools.partial(body, mesh.shape["row"], mesh.shape["col"]),
        mesh=mesh,
        in_specs=placed,
        out_specs=(P(("row", "col")), P(None, ("row", "col"), None)),
        check_vma=False,
    )
```
